16 devices in a mesh: dp: 4 (over y, z, core), tp: 4 (over x).
Axes of the slice: x: 4, y: 2, z: 1, core: 2. Of those that a mesh axis runs over, the one named last changes fastest.
The devices are a block of a 4x4x8 slice.
Arguments:
- x: bfloat16 [2048, 8192], P(('dp', 'tp')), parts along dimension 0
- gain_a: bfloat16 [8192], replicated
- wq: bfloat16 [8192, 8192], P(None, 'tp')
- wk: bfloat16 [8192, 1024], P(None, 'tp')
- wv: bfloat16 [8192, 1024], P(None, 'tp')
- wo: bfloat16 [8192, 8192], P('tp')
- gain_m: bfloat16 [8192], replicated
- w_gate: bfloat16 [8192, 22016], P(None, 'tp')
- w_up: bfloat16 [8192, 22016], P(None, 'tp')
- w_down: bfloat16 [22016, 8192], P('tp')
Outputs:
- output: bfloat16 [2048, 8192], P(('dp', 'tp')), parts along dimension 0
There are 4 independent parts. The reference program is written for one: setup_inputs(seed, part) draws one part's arguments, and reference() takes and returns one part's arrays. A program takes and returns all parts, laid end to end along the dimension named above; an argument that names none is the same for every part.
All inputs are finite; a program needn't handle non-finite values.
Results may differ from the reference program's by a relative error of at most 0.017.
Values are sent between devices in bfloat16 or wider.
A program may use at most 768 MiB of HBM per device.

```python
import jax
import jax.numpy as jnp
from jax import lax

ROWS = 512
D = 8192
HEADS = 64
KV_HEADS = 8
HEAD = 128
FF = 22016
THETA = 10000


def setup_inputs(seed: int = 0, part: int = 0) -> dict:
    kx, kn, kq, kk, kv, ko, km, kg, ku, kd = jax.random.split(jax.random.key(seed), 10)

    def weights(key, rows, columns):
        return jax.random.normal(key, (rows, columns), jnp.float32) * rows**-0.5

    drawn = {
        "x": jax.random.normal(jax.random.fold_in(kx, part), (ROWS, D), jnp.float32),
        "gain_a": 1 + 0.1 * jax.random.normal(kn, (D,), jnp.float32),
        "wq": 2 * weights(kq, D, HEADS * HEAD),
        "wk": 2 * weights(kk, D, KV_HEADS * HEAD),
        "wv": 4 * weights(kv, D, KV_HEADS * HEAD),
        "wo": weights(ko, HEADS * HEAD, D),
        "gain_m": 1 + 0.1 * jax.random.normal(km, (D,), jnp.float32),
        "w_gate": weights(kg, D, FF),
        "w_up": weights(ku, D, FF),
        "w_down": 2 * weights(kd, FF, D),
    }
    return {k: v.astype(jnp.bfloat16) for k, v in drawn.items()}


def normed(x, gain):
    wide = x.astype(jnp.float32)
    scale = lax.rsqrt(jnp.mean(wide * wide, -1, keepdims=True) + 1e-6)
    return (wide * scale * gain.astype(jnp.float32)).astype(jnp.bfloat16)


def turned(t, place, theta):
    half = t.shape[-1] // 2
    angle = place.astype(jnp.float32)[:, None] * theta ** (-jnp.arange(half, dtype=jnp.float32) / half)
    cos, sin = jnp.cos(angle)[:, None], jnp.sin(angle)[:, None]
    a, b = t[..., :half].astype(jnp.float32), t[..., half:].astype(jnp.float32)
    return jnp.concatenate([a * cos - b * sin, b * cos + a * sin], -1).astype(jnp.bfloat16)


def matmul(a, w):
    return jnp.dot(a, w, preferred_element_type=jnp.float32).astype(jnp.bfloat16)


def einsum(form, a, b):
    return jnp.einsum(form, a.astype(jnp.float32), b.astype(jnp.float32))


def attention(q, k, v):
    scores = einsum("tgsd,ugd->gstu", q, k) * q.shape[-1] ** -0.5
    token = jnp.arange(q.shape[0])
    scores = jnp.where(token[:, None] >= token, scores, -jnp.inf)
    weights = jax.nn.softmax(scores, -1).astype(jnp.bfloat16)
    return einsum("gstu,ugd->tgsd", weights, v).astype(jnp.bfloat16)


def reference(x, gain_a, wq, wk, wv, wo, gain_m, w_gate, w_up, w_down):
    a, place = normed(x, gain_a), jnp.arange(ROWS)
    q = turned(matmul(a, wq).reshape(ROWS, HEADS, HEAD), place, THETA).reshape(ROWS, KV_HEADS, -1, HEAD)
    k = turned(matmul(a, wk).reshape(ROWS, KV_HEADS, HEAD), place, THETA)
    v = matmul(a, wv).reshape(ROWS, KV_HEADS, HEAD)
    seen = attention(q, k, v).reshape(ROWS, HEADS * HEAD)
    h = (x.astype(jnp.float32) + jnp.dot(seen, wo, preferred_element_type=jnp.float32)).astype(jnp.bfloat16)
    b = normed(h, gain_m)
    gate = jnp.dot(b, w_gate, preferred_element_type=jnp.float32)
    up = jnp.dot(b, w_up, preferred_element_type=jnp.float32)
    hidden = (jax.nn.silu(gate) * up).astype(jnp.bfloat16)
    return (h.astype(jnp.float32) + jnp.dot(hidden, w_down, preferred_element_type=jnp.float32)).astype(jnp.bfloat16)
```

```python
import functools

import jax
import jax.numpy as jnp
from jax import lax
from jax.experimental import pallas as pl
from jax.experimental.pallas import tpu as pltpu
from jax.sharding import PartitionSpec as P

HEAD = 128
THETA = 10000
BF, F32 = jnp.bfloat16, jnp.float32
ANY = pl.BlockSpec(memory_space=pl.ANY)
VM = pl.BlockSpec(memory_space=pltpu.VMEM)
CH = 1024
TN = 512
HALF = TN // 2
VMEM = 63 * 2**20


def _dot(a, b, ca=1, cb=0):
    return lax.dot_general(a, b, (((ca,), (cb,)), ((), ())), preferred_element_type=F32)


def _ring(n):
    me = lax.axis_index("tp")
    return me, lax.rem(me + 1, n), lax.rem(me + n - 1, n), lax.rem(me + 2, n)


def _greet(right, left):
    barrier = pltpu.get_barrier_semaphore()
    for at in (left, right):
        pl.semaphore_signal(barrier, inc=1, device_id={"tp": at}, device_id_type=pl.DeviceIdType.MESH)
    pl.semaphore_wait(barrier, 2)


def _send(src, dst, ssem, rsem, to):
    return pltpu.make_async_remote_copy(src_ref=src, dst_ref=dst, send_sem=ssem, recv_sem=rsem, device_id={"tp": to},
                                        device_id_type=pl.DeviceIdType.MESH)


def _loop(a, b, body):
    lax.fori_loop(a, b, lambda i, _: (body(i), None)[1], None)


def _norm_into(x_ref, gain_ref, buf, me, rows):
    chunks = buf.shape[0]
    wide = chunks * CH

    def body(i):
        at = pl.ds(pl.multiple_of(i * 16, 16), 16)
        total = jnp.zeros((16, CH), F32)
        for c in range(chunks):
            t = x_ref[at, c * CH : (c + 1) * CH].astype(F32)
            total = total + t * t
        scale = lax.rsqrt(jnp.sum(total, -1, keepdims=True) * (1.0 / wide) + 1e-6)
        to = pl.ds(pl.multiple_of(me * rows + i * 16, 16), 16)
        for c in range(chunks):
            t = x_ref[at, c * CH : (c + 1) * CH].astype(F32)
            buf[c, to, :] = (t * scale * gain_ref[:, c * CH : (c + 1) * CH].astype(F32)).astype(BF)

    _loop(0, rows // 16, body)


class _Gather:
    def __init__(self, n, rows, buf, sems):
        self.me, self.right, self.left, self.opp = _ring(n)
        self.rows, self.buf = rows, buf
        self.s_own, self.r_own, self.s_fwd, self.r_fwd = sems

    def _own(self, c, way):
        at = self.buf.at[c, pl.ds(pl.multiple_of(self.me * self.rows, 128), self.rows), :]
        return _send(at, at, self.s_own.at[way, c], self.r_own.at[way, c], self.left if way else self.right)

    def _fwd(self, c, way):
        half = self.rows // 2
        source = self.right if way else self.left
        at = self.buf.at[c, pl.ds(pl.multiple_of(source * self.rows + way * half, half), half), :]
        return _send(at, at, self.s_fwd.at[way, c], self.r_fwd.at[way, c], self.left if way else self.right)

    def start(self, c):
        self._own(c, 0).start()
        self._own(c, 1).start()

    def forward(self, c):
        self._own(c, 0).wait_recv()
        self._fwd(c, 0).start()
        self._own(c, 1).wait_recv()
        self._fwd(c, 1).start()

    def whole(self, c):
        self._fwd(c, 0).wait_recv()
        self._fwd(c, 1).wait_recv()

    def end(self):
        def body(c):
            for way in (0, 1):
                self._own(c, way).wait_send()
                self._fwd(c, way).wait_send()

        _loop(0, self.buf.shape[0], body)


def _attention_kernel(n, x_ref, gain_ref, cos_ref, sin_ref, wq_ref, wk_ref, wv_ref, seen_ref,
                      buf, acc, w_s, qkv_s, w_sem, s_own, r_own, s_fwd, r_fwd):
    rows = x_ref.shape[0]
    chunks, slots = buf.shape[0], w_s.shape[0]
    nq, nk = wq_ref.shape[1], wk_ref.shape[1]
    tokens = n * rows
    total = nq + 2 * nk
    g = _Gather(n, rows, buf, (s_own, r_own, s_fwd, r_fwd))

    def weights(c, slot):
        at = pl.ds(pl.multiple_of(c * CH, CH), CH)
        return [pltpu.make_async_copy(ref.at[at, :], w_s.at[slot, :, lo : lo + size], w_sem.at[slot, i])
                for i, (ref, lo, size) in enumerate(((wq_ref, 0, nq), (wk_ref, nq, nk), (wv_ref, nq + nk, nk)))]

    for c in range(slots):
        for copy in weights(c, c):
            copy.start()
    _norm_into(x_ref, gain_ref, buf, g.me, rows)
    _greet(g.right, g.left)
    g.start(0)
    g.start(1)
    acc[...] = jnp.zeros_like(acc)
    g.forward(0)

    def chunk(c):
        @pl.when(c + 2 < chunks)
        def _():
            g.start(c + 2)

        @pl.when(c + 1 < chunks)
        def _():
            g.forward(c + 1)

        g.whole(c)
        slot = lax.rem(c, slots)
        for copy in weights(c, slot):
            copy.wait()

        def tile(j):
            at = pl.ds(pl.multiple_of(j * 256, 256), 256)
            acc[:, at] += _dot(buf[c], w_s[slot, :, at])

        _loop(0, total // 256, tile)

        @pl.when(c + slots < chunks)
        def _():
            for copy in weights(c + slots, slot):
                copy.start()

    _loop(0, chunks, chunk)

    def turned(at):
        t = acc[:, at].astype(BF).astype(F32)
        return (t * cos_ref[...] + pltpu.roll(t, HEAD // 2, 1) * sin_ref[...]).astype(BF)

    kv = nk // HEAD
    for i in range(kv):
        qkv_s[i] = turned(slice(nq + i * HEAD, nq + (i + 1) * HEAD))
        qkv_s[kv + i] = acc[:, nq + nk + i * HEAD : nq + nk + (i + 1) * HEAD].astype(BF)
    group = nq // nk
    bq = 128
    hidden = lax.broadcasted_iota(jnp.int32, (bq, bq), 0) < lax.broadcasted_iota(jnp.int32, (bq, bq), 1)

    def head(h):
        at = pl.ds(pl.multiple_of(h * HEAD, HEAD), HEAD)
        q = turned(at)
        i = lax.div(h, group)
        for b in range(tokens // bq):
            seen = (b + 1) * bq
            s = _dot(q[b * bq : seen, :], qkv_s[i, :seen, :], 1, 1) * (HEAD**-0.5)
            last = jnp.where(hidden, -1e30, s[:, b * bq :])
            s = jnp.concatenate([s[:, : b * bq], last], 1) if b else last
            p = jnp.exp(s - jnp.max(s, -1, keepdims=True))
            out = _dot(p.astype(BF), qkv_s[kv + i, :seen, :]) / jnp.sum(p, -1, keepdims=True)
            seen_ref[b * bq : seen, at] = out.astype(BF)

    _loop(0, nq // HEAD, head)
    g.end()


def attention(n, x, gain, cos, sin, wq, wk, wv):
    rows, d = x.shape
    nq, nk = wq.shape[1], wk.shape[1]
    chunks = d // CH
    slots = 3
    return pl.pallas_call(
        functools.partial(_attention_kernel, n),
        out_shape=jax.ShapeDtypeStruct((n * rows, nq), BF),
        in_specs=[VM, VM, VM, VM, ANY, ANY, ANY],
        out_specs=VM,
        scratch_shapes=[
            pltpu.VMEM((chunks, n * rows, CH), BF),
            pltpu.VMEM((n * rows, nq + 2 * nk), F32),
            pltpu.VMEM((slots, CH, nq + 2 * nk), BF),
            pltpu.VMEM((2 * nk // HEAD, n * rows, HEAD), BF),
            pltpu.SemaphoreType.DMA((slots, 3)),
        ] + [pltpu.SemaphoreType.DMA((2, chunks))] * 4,
        compiler_params=pltpu.CompilerParams(collective_id=0, has_side_effects=True, vmem_limit_bytes=VMEM),
        name="gather_attention",
    )(x, gain.reshape(1, -1), cos, sin, wq, wk, wv)


def _hidden_kernel(n, x_ref, gain_ref, wg_ref, wu_ref, out_ref, buf, acc, w_s, w_sem, s_own, r_own, s_fwd, r_fwd):
    rows = x_ref.shape[0]
    chunks, slots = buf.shape[0], w_s.shape[0]
    tiles = wg_ref.shape[1] // 128
    steps = chunks * tiles
    g = _Gather(n, rows, buf, (s_own, r_own, s_fwd, r_fwd))

    def weights(s):
        slot, c, j = lax.rem(s, slots), lax.div(s, tiles), lax.rem(s, tiles)
        at = pl.ds(pl.multiple_of(c * CH, CH), CH), pl.ds(pl.multiple_of(j * 128, 128), 128)
        return [pltpu.make_async_copy(ref.at[at], w_s.at[slot, :, i * 128 : (i + 1) * 128], w_sem.at[slot, i])
                for i, ref in enumerate((wg_ref, wu_ref))]

    def fetch(s):
        for copy in weights(s):
            copy.start()

    _loop(0, slots, fetch)
    _norm_into(x_ref, gain_ref, buf, g.me, rows)
    _greet(g.right, g.left)
    g.start(0)
    g.start(1)

    def clear(j):
        acc[j] = jnp.zeros(acc.shape[1:], F32)

    _loop(0, tiles, clear)
    g.forward(0)

    def product(c, j):
        s = c * tiles + j
        for copy in weights(s):
            copy.wait()
        value = acc[j] + _dot(buf[c], w_s[lax.rem(s, slots)])

        @pl.when(s + slots < steps)
        def _():
            fetch(s + slots)

        return value

    def chunk(c):
        @pl.when(c + 2 < chunks)
        def _():
            g.start(c + 2)

        g.forward(c + 1)
        g.whole(c)

        def tile(j):
            acc[j] = product(c, j)

        _loop(0, tiles, tile)

    _loop(0, chunks - 1, chunk)
    g.whole(chunks - 1)

    def last(j):
        t = product(chunks - 1, j)
        gate, up = t[:, :128], t[:, 128:]
        out_ref[:, pl.ds(pl.multiple_of(j * 128, 128), 128)] = (gate * jax.nn.sigmoid(gate) * up).astype(BF)

    _loop(0, tiles, last)
    g.end()


def hidden_units(n, x, gain, wg, wu):
    rows, d = x.shape
    chunks, tiles, slots = d // CH, wg.shape[1] // 128, 12
    return pl.pallas_call(
        functools.partial(_hidden_kernel, n),
        out_shape=jax.ShapeDtypeStruct((n * rows, wg.shape[1]), BF),
        in_specs=[VM, VM, ANY, ANY],
        out_specs=VM,
        scratch_shapes=[
            pltpu.VMEM((chunks, n * rows, CH), BF),
            pltpu.VMEM((tiles, n * rows, 256), F32),
            pltpu.VMEM((slots, CH, 256), BF),
            pltpu.SemaphoreType.DMA((slots, 2)),
        ] + [pltpu.SemaphoreType.DMA((2, chunks))] * 4,
        compiler_params=pltpu.CompilerParams(collective_id=1, has_side_effects=True, vmem_limit_bytes=VMEM),
        name="gather_hidden",
    )(x, gain.reshape(1, -1), wg, wu)


def _scatter_kernel(n, act_ref, rest_ref, w_ref, out_ref, w_s, part, own, s_opp, r_opp, s_near, r_near,
                    w_sem, ss_opp, rs_opp, ss_near, rs_near):
    rows = rest_ref.shape[0]
    chunks, slots = own.shape[0], w_s.shape[0]
    me, right, left, opp = _ring(n)

    def weights(j):
        slot = lax.rem(j, slots)
        return pltpu.make_async_copy(w_ref.at[:, pl.ds(pl.multiple_of(j * TN, TN), TN)], w_s.at[slot], w_sem.at[slot])

    def far(j, way):
        return _send(s_opp.at[way, j], r_opp.at[way, j], ss_opp.at[way, j], rs_opp.at[way, j], left if way else right)

    def near(j, way):
        return _send(s_near.at[way, j], r_near.at[way, j], ss_near.at[way, j], rs_near.at[way, j], left if way else right)

    def of(device):
        return pl.ds(pl.multiple_of(device * rows, rows), rows)

    def pass_on(j):
        at = lax.rem(j, 2)
        for way, device in ((0, right), (1, left)):
            far(j, way).wait_recv()
            t = part[at, of(device), :]
            came = r_opp[way, j].astype(F32)
            a, b = t[:, :HALF], t[:, HALF:]
            if way:
                b = b + came
            else:
                a = a + came
            s_near[way, j, :, :HALF] = a.astype(BF)
            s_near[way, j, :, HALF:] = b.astype(BF)
            near(j, way).start()

    for j in range(slots):
        weights(j).start()
    _greet(right, left)

    def chunk(j):
        weights(j).wait()
        at, slot = lax.rem(j, 2), lax.rem(j, slots)
        for i in range(TN // 256):
            part[at, :, i * 256 : (i + 1) * 256] = _dot(act_ref[...], w_s[slot, :, i * 256 : (i + 1) * 256])

        @pl.when(j + slots < chunks)
        def _():
            weights(j + slots).start()

        t = part[at, of(opp), :]
        for way in (0, 1):
            s_opp[way, j] = t[:, way * HALF : (way + 1) * HALF].astype(BF)
            far(j, way).start()
        own[j] = part[at, of(me), :]

        @pl.when(j > 0)
        def _():
            pass_on(j - 1)

    _loop(0, chunks, chunk)
    pass_on(chunks - 1)

    def finish(j):
        near(j, 0).wait_recv()
        near(j, 1).wait_recv()
        at = pl.ds(pl.multiple_of(j * TN, TN), TN)
        total = own[j] + r_near[0, j].astype(F32) + r_near[1, j].astype(F32)
        out_ref[:, at] = (rest_ref[:, at].astype(F32) + total).astype(BF)
        for way in (0, 1):
            far(j, way).wait_send()
            near(j, way).wait_send()

    _loop(0, chunks, finish)


def added(n, rest, act, w, ident):
    rows, d = rest.shape
    chunks, slots = d // TN, 3
    return pl.pallas_call(
        functools.partial(_scatter_kernel, n),
        out_shape=jax.ShapeDtypeStruct((rows, d), BF),
        in_specs=[VM, VM, ANY],
        out_specs=VM,
        scratch_shapes=[
            pltpu.VMEM((slots, w.shape[0], TN), BF),
            pltpu.VMEM((2, n * rows, TN), F32),
            pltpu.VMEM((chunks, rows, TN), F32),
            pltpu.VMEM((2, chunks, rows, HALF), BF),
            pltpu.VMEM((2, chunks, rows, HALF), BF),
            pltpu.VMEM((2, chunks, rows, TN), BF),
            pltpu.VMEM((2, chunks, rows, TN), BF),
            pltpu.SemaphoreType.DMA((slots,)),
        ] + [pltpu.SemaphoreType.DMA((2, chunks))] * 4,
        compiler_params=pltpu.CompilerParams(collective_id=ident, has_side_effects=True, vmem_limit_bytes=VMEM),
        name=f"scatter_{ident}",
    )(act, rest, w)


def solution(mesh):
    n = mesh.shape["tp"]

    def step(x, gain_a, wq, wk, wv, wo, gain_m, w_gate, w_up, w_down):
        half = HEAD // 2
        angle = jnp.arange(n * x.shape[0], dtype=F32)[:, None] * THETA ** (-jnp.arange(half, dtype=F32) / half)
        cos, sin = jnp.cos(angle), jnp.sin(angle)
        seen = attention(n, x, gain_a, jnp.concatenate([cos, cos], 1), jnp.concatenate([-sin, sin], 1), wq, wk, wv)
        h = added(n, x, seen, wo, 2)
        hidden = hidden_units(n, h, gain_m, w_gate, w_up)
        return added(n, h, hidden, w_down, 3)

    tokens, columns, rows_of = P(("dp", "tp"), None), P(None, "tp"), P("tp", None)
    return jax.shard_map(
        step,
        mesh=mesh,
        in_specs=(tokens, P(None), columns, columns, columns, rows_of, P(None), columns, columns, rows_of),
        out_specs=tokens,
        check_vma=False,
    )
```

```python
import functools

import jax
import jax.numpy as jnp
import numpy as np
from jax import lax
from jax.experimental import pallas as pl
from jax.experimental.pallas import tpu as pltpu
from jax.sharding import PartitionSpec as P

HEAD = 128
THETA = 10000
BF, F32 = jnp.bfloat16, jnp.float32
ANY = pl.BlockSpec(memory_space=pl.ANY)
VM = pl.BlockSpec(memory_space=pltpu.VMEM)
CH = 1024
TN = 512
HALF = TN // 2
GROUP = 9
LEAD = 5
HOLD = 12
AHEAD = 2
LAG = 2
VMEM = 63 * 2**20


def _dot(a, b, ca=1, cb=0):
    return lax.dot_general(a, b, (((ca,), (cb,)), ((), ())), preferred_element_type=F32)


def _ring(n):
    me = lax.axis_index("tp")
    return me, lax.rem(me + 1, n), lax.rem(me + n - 1, n), lax.rem(me + 2, n)


def _greet(right, left, other=None, also=0):
    barrier = pltpu.get_barrier_semaphore()
    for at in (left, right):
        pl.semaphore_signal(barrier, inc=1, device_id={"tp": at}, device_id_type=pl.DeviceIdType.MESH)
    if other is not None:
        pl.semaphore_signal(barrier, inc=1, device_id={"dp": other}, device_id_type=pl.DeviceIdType.MESH)
    pl.semaphore_wait(barrier, (2 if other is None else 3) + also)


def _send(src, dst, ssem, rsem, to):
    return pltpu.make_async_remote_copy(src_ref=src, dst_ref=dst, send_sem=ssem, recv_sem=rsem, device_id={"tp": to},
                                        device_id_type=pl.DeviceIdType.MESH)


def _loop(a, b, body):
    lax.fori_loop(a, b, lambda i, _: (body(i), None)[1], None)


def _norm_into(x_ref, gain_ref, buf, me, rows):
    chunks = buf.shape[0]
    wide = chunks * CH
    gain = [gain_ref[c * CH : (c + 1) * CH].astype(F32).reshape(1, CH) for c in range(chunks)]

    def body(i):
        at = pl.ds(pl.multiple_of(i * 16, 16), 16)
        total = jnp.zeros((16, CH), F32)
        for c in range(chunks):
            t = x_ref[at, c * CH : (c + 1) * CH].astype(F32)
            total = total + t * t
        scale = lax.rsqrt(jnp.sum(total, -1, keepdims=True) * (1.0 / wide) + 1e-6)
        to = pl.ds(pl.multiple_of(me * rows + i * 16, 16), 16)
        for c in range(chunks):
            t = x_ref[at, c * CH : (c + 1) * CH].astype(F32)
            buf[c, to, :] = (t * scale * gain[c]).astype(BF)

    _loop(0, rows // 16, body)


class _Gather:
    def __init__(self, n, rows, buf, sems):
        self.me, self.right, self.left, self.opp = _ring(n)
        self.rows, self.buf = rows, buf
        self.s_own, self.r_own, self.s_fwd, self.r_fwd = sems

    def _own(self, c, way):
        at = self.buf.at[c, pl.ds(pl.multiple_of(self.me * self.rows, 128), self.rows), :]
        return _send(at, at, self.s_own.at[way, c], self.r_own.at[way, c], self.left if way else self.right)

    def _fwd(self, c, way):
        half = self.rows // 2
        source = self.right if way else self.left
        at = self.buf.at[c, pl.ds(pl.multiple_of(source * self.rows + way * half, half), half), :]
        return _send(at, at, self.s_fwd.at[way, c], self.r_fwd.at[way, c], self.left if way else self.right)

    def start(self, c):
        self._own(c, 0).start()
        self._own(c, 1).start()

    def forward(self, c):
        self._own(c, 0).wait_recv()
        self._fwd(c, 0).start()
        self._own(c, 1).wait_recv()
        self._fwd(c, 1).start()

    def whole(self, c):
        self._fwd(c, 0).wait_recv()
        self._fwd(c, 1).wait_recv()

    def end(self):
        def body(c):
            for way in (0, 1):
                self._own(c, way).wait_send()
                self._fwd(c, way).wait_send()

        _loop(0, self.buf.shape[0], body)


def _attention_kernel(n, x_ref, gain_ref, cos_ref, sin_ref, wq_ref, wk_ref, wv_ref, seen_ref,
                      buf, acc, w_s, qkv_s, w_sem, go, s_own, r_own, s_fwd, r_fwd):
    group_id = lax.axis_index("dp")
    second = lax.rem(group_id, 2)
    other = group_id + 1 - 2 * second
    rows = x_ref.shape[0]
    chunks, slots = buf.shape[0], w_s.shape[0]
    nq, nk = wq_ref.shape[1], wk_ref.shape[1]
    tokens = n * rows
    total = nq + 2 * nk
    g = _Gather(n, rows, buf, (s_own, r_own, s_fwd, r_fwd))

    def weights(c, slot):
        at = pl.ds(pl.multiple_of(c * CH, CH), CH)
        return [pltpu.make_async_copy(ref.at[at, :], w_s.at[slot, :, lo : lo + size], w_sem.at[slot, i])
                for i, (ref, lo, size) in enumerate(((wq_ref, 0, nq), (wk_ref, nq, nk), (wv_ref, nq + nk, nk)))]

    for c in range(slots):
        for copy in weights(c, c):
            copy.start()
    _norm_into(x_ref, gain_ref, buf, g.me, rows)
    acc[...] = jnp.zeros_like(acc)
    _greet(g.right, g.left, other)

    @pl.when(second == 1)
    def _():
        pl.semaphore_wait(go, 1)

    for c in range(AHEAD + 2):
        g.start(c)
    for c in range(AHEAD):
        g.forward(c)

    def chunk(c):
        @pl.when(c + AHEAD + 2 < chunks)
        def _():
            g.start(c + AHEAD + 2)

        @pl.when(c + AHEAD < chunks)
        def _():
            g.forward(c + AHEAD)

        g.whole(c)

        @pl.when((second == 0) & (c == LEAD))
        def _():
            pl.semaphore_signal(go, inc=1, device_id={"dp": other}, device_id_type=pl.DeviceIdType.MESH)

        slot = lax.rem(c, slots)
        for copy in weights(c, slot):
            copy.wait()

        for lo in range(0, total, 256):
            acc[:, lo : lo + 256] += _dot(buf[c], w_s[slot, :, lo : lo + 256])

        @pl.when(c + slots < chunks)
        def _():
            for copy in weights(c + slots, slot):
                copy.start()

    _loop(0, chunks, chunk)

    def turned(at, of=slice(None)):
        t = acc[of, at].astype(BF).astype(F32)
        return (t * cos_ref[of, :] + pltpu.roll(t, HEAD // 2, 1) * sin_ref[of, :]).astype(BF)

    kv = nk // HEAD
    for i in range(kv):
        qkv_s[i] = turned(slice(nq + i * HEAD, nq + (i + 1) * HEAD))
        qkv_s[kv + i] = acc[:, nq + nk + i * HEAD : nq + nk + (i + 1) * HEAD].astype(BF)
    group = nq // nk
    bq = 128
    hidden = lax.broadcasted_iota(jnp.int32, (bq, bq), 0) < lax.broadcasted_iota(jnp.int32, (bq, bq), 1)

    def heads(pair):
        at = pl.ds(pl.multiple_of(pair * 2 * HEAD, 2 * HEAD), 2 * HEAD)
        i = lax.div(pair * 2, group)
        for b in range(tokens // bq):
            seen = (b + 1) * bq
            outs = []
            for t in range(2):
                q = turned(pl.ds(pl.multiple_of((pair * 2 + t) * HEAD, HEAD), HEAD), slice(b * bq, seen))
                s = _dot(q, qkv_s[i, :seen, :], 1, 1) * (HEAD**-0.5)
                last = jnp.where(hidden, -1e30, s[:, b * bq :])
                s = jnp.concatenate([s[:, : b * bq], last], 1) if b else last
                p = jnp.exp(s - jnp.max(s, -1, keepdims=True))
                out = _dot(p.astype(BF), qkv_s[kv + i, :seen, :]) / jnp.sum(p, -1, keepdims=True)
                outs.append(out.astype(BF))
            seen_ref[b * bq : seen, at] = jnp.concatenate(outs, 1)

    _loop(0, nq // (2 * HEAD), heads)
    g.end()


def attention(n, x, gain, cos, sin, wq, wk, wv):
    rows, d = x.shape
    nq, nk = wq.shape[1], wk.shape[1]
    chunks = d // CH
    slots = 3
    return pl.pallas_call(
        functools.partial(_attention_kernel, n),
        out_shape=jax.ShapeDtypeStruct((n * rows, nq), BF),
        in_specs=[VM, VM, VM, VM, ANY, ANY, ANY],
        out_specs=VM,
        scratch_shapes=[
            pltpu.VMEM((chunks, n * rows, CH), BF),
            pltpu.VMEM((n * rows, nq + 2 * nk), F32),
            pltpu.VMEM((slots, CH, nq + 2 * nk), BF),
            pltpu.VMEM((2 * nk // HEAD, n * rows, HEAD), BF),
            pltpu.SemaphoreType.DMA((slots, 3)),
            pltpu.SemaphoreType.REGULAR,
        ] + [pltpu.SemaphoreType.DMA((2, chunks))] * 4,
        compiler_params=pltpu.CompilerParams(collective_id=0, has_side_effects=True, vmem_limit_bytes=VMEM),
        name="gather_attention",
    )(x, gain, cos, sin, wq, wk, wv)


def _hidden_kernel(n, x_ref, gain_ref, wg_ref, wu_ref, out_ref, buf, acc, w_s, w_sem, s_own, r_own, s_fwd, r_fwd):
    rows = x_ref.shape[0]
    chunks, slots = buf.shape[0], w_s.shape[0]
    full, rest = divmod(wg_ref.shape[1] // 128, GROUP)
    per = full + (rest > 0)
    steps = chunks * per
    g = _Gather(n, rows, buf, (s_own, r_own, s_fwd, r_fwd))

    def weights(s, tiles):
        slot, c, i = lax.rem(s, slots), lax.div(s, per), lax.rem(s, per)
        at = pl.ds(pl.multiple_of(c * CH, CH), CH), pl.ds(pl.multiple_of(i * GROUP * 128, 128), tiles * 128)
        return [pltpu.make_async_copy(ref.at[at], w_s.at[slot, k, :, : tiles * 128], w_sem.at[slot, k])
                for k, ref in enumerate((wg_ref, wu_ref))]

    def fetch(s):
        for yes, tiles in ((lax.rem(s, per) < full, GROUP), (lax.rem(s, per) == full, rest)):
            if tiles:
                @pl.when((s < steps) & yes)
                def _():
                    for copy in weights(s, tiles):
                        copy.start()

    _loop(0, slots, fetch)
    _norm_into(x_ref, gain_ref, buf, g.me, rows)
    _greet(g.right, g.left)
    g.start(0)

    def clear(j):
        acc[j] = jnp.zeros(acc.shape[1:], F32)

    _loop(0, acc.shape[0], clear)
    g.forward(0)
    g.start(1)
    g.start(2)
    g.forward(1)

    def products(c, i, tiles, done):
        s = c * per + i
        slot = lax.rem(s, slots)
        for copy in weights(s, tiles):
            copy.wait()
        for t in range(tiles):
            cols = slice(t * 128, (t + 1) * 128)
            w = jnp.concatenate([w_s[slot, 0, :, cols], w_s[slot, 1, :, cols]], 1)
            j = i * GROUP + t
            done(j, acc[j] + _dot(buf[c], w))
        fetch(s + slots)

    def groups(c, done):
        _loop(0, full, lambda i: products(c, i, GROUP, done))
        if rest:
            products(c, full, rest, done)

    def chunk(c):
        @pl.when(c + 3 < chunks)
        def _():
            g.start(c + 3)

        @pl.when(c + 2 < chunks)
        def _():
            g.forward(c + 2)

        g.whole(c)

        def keep(j, value):
            acc[j] = value

        groups(c, keep)

    _loop(0, chunks - 1, chunk)
    g.whole(chunks - 1)

    def last(j, value):
        gate, up = value[:, :128], value[:, 128:]
        out_ref[:, pl.ds(pl.multiple_of(j * 128, 128), 128)] = (gate * jax.nn.sigmoid(gate) * up).astype(BF)

    groups(chunks - 1, last)
    g.end()


def hidden_units(n, x, gain, wg, wu):
    rows, d = x.shape
    chunks, tiles, slots = d // CH, wg.shape[1] // 128, 3
    return pl.pallas_call(
        functools.partial(_hidden_kernel, n),
        out_shape=jax.ShapeDtypeStruct((n * rows, wg.shape[1]), BF),
        in_specs=[VM, VM, ANY, ANY],
        out_specs=VM,
        scratch_shapes=[
            pltpu.VMEM((chunks, n * rows, CH), BF),
            pltpu.VMEM((tiles, n * rows, 256), F32),
            pltpu.VMEM((slots, 2, CH, GROUP * 128), BF),
            pltpu.SemaphoreType.DMA((slots, 2)),
        ] + [pltpu.SemaphoreType.DMA((2, chunks))] * 4,
        compiler_params=pltpu.CompilerParams(collective_id=1, has_side_effects=True, vmem_limit_bytes=VMEM),
        name="gather_hidden",
    )(x, gain, wg, wu)


def _scatter_kernel(n, act_ref, rest_ref, w_ref, out_ref, w_s, part, own, s_opp, r_opp, s_near, r_near,
                    w_sem, go, ss_opp, rs_opp, ss_near, rs_near, *, paired):
    group_id = lax.axis_index("dp")
    second = lax.rem(group_id, 2)
    other = group_id + 1 - 2 * second
    rows = rest_ref.shape[0]
    chunks, slots = own.shape[0], w_s.shape[0]
    me, right, left, opp = _ring(n)

    def weights(j):
        slot = lax.rem(j, slots)
        return pltpu.make_async_copy(w_ref.at[:, pl.ds(pl.multiple_of(j * TN, TN), TN)], w_s.at[slot], w_sem.at[slot])

    def far(j, way):
        return _send(s_opp.at[way, j], r_opp.at[way, j], ss_opp.at[way, j], rs_opp.at[way, j], left if way else right)

    def near(j, way):
        return _send(s_near.at[way, j], r_near.at[way, j], ss_near.at[way, j], rs_near.at[way, j], left if way else right)

    def of(device):
        return pl.ds(pl.multiple_of(device * rows, rows), rows)

    def pass_on(j):
        at = lax.rem(j, LAG + 1)
        for way, device in ((0, right), (1, left)):
            far(j, way).wait_recv()
            t = part[at, of(device), :]
            came = r_opp[way, j].astype(F32)
            a, b = t[:, :HALF], t[:, HALF:]
            if way:
                b = b + came
            else:
                a = a + came
            s_near[way, j, :, :HALF] = a.astype(BF)
            s_near[way, j, :, HALF:] = b.astype(BF)
            near(j, way).start()

    for j in range(slots):
        weights(j).start()
    if paired:
        @pl.when(second == 0)
        def _():
            pl.semaphore_signal(pltpu.get_barrier_semaphore(), inc=1, device_id={"dp": other}, device_id_type=pl.DeviceIdType.MESH)
    _greet(right, left, also=second if paired else 0)

    def chunk(j):
        if paired:
            @pl.when((second == 1) & (j == HOLD))
            def _():
                pl.semaphore_signal(go, inc=1, device_id={"dp": other}, device_id_type=pl.DeviceIdType.MESH)
        weights(j).wait()
        at, slot = lax.rem(j, LAG + 1), lax.rem(j, slots)
        for i in range(TN // 256):
            part[at, :, i * 256 : (i + 1) * 256] = _dot(act_ref[...], w_s[slot, :, i * 256 : (i + 1) * 256])

        @pl.when(j + slots < chunks)
        def _():
            weights(j + slots).start()

        t = part[at, of(opp), :]
        for way in (0, 1):
            s_opp[way, j] = t[:, way * HALF : (way + 1) * HALF].astype(BF)
            far(j, way).start()
        own[j] = part[at, of(me), :]

        @pl.when(j >= LAG)
        def _():
            pass_on(j - LAG)

    _loop(0, chunks, chunk)
    _loop(chunks - LAG, chunks, pass_on)

    def finish(j):
        near(j, 0).wait_recv()
        near(j, 1).wait_recv()
        at = pl.ds(pl.multiple_of(j * TN, TN), TN)
        total = own[j] + r_near[0, j].astype(F32) + r_near[1, j].astype(F32)
        out_ref[:, at] = (rest_ref[:, at].astype(F32) + total).astype(BF)
        for way in (0, 1):
            far(j, way).wait_send()
            near(j, way).wait_send()

    _loop(0, chunks, finish)
    if paired:
        @pl.when(second == 0)
        def _():
            pl.semaphore_wait(go, 1)


def added(n, rest, act, w, ident, paired=False):
    rows, d = rest.shape
    chunks, slots = d // TN, 3
    return pl.pallas_call(
        functools.partial(_scatter_kernel, n, paired=paired),
        out_shape=jax.ShapeDtypeStruct((rows, d), BF),
        in_specs=[VM, VM, ANY],
        out_specs=VM,
        scratch_shapes=[
            pltpu.VMEM((slots, w.shape[0], TN), BF),
            pltpu.VMEM((LAG + 1, n * rows, TN), F32),
            pltpu.VMEM((chunks, rows, TN), F32),
            pltpu.VMEM((2, chunks, rows, HALF), BF),
            pltpu.VMEM((2, chunks, rows, HALF), BF),
            pltpu.VMEM((2, chunks, rows, TN), BF),
            pltpu.VMEM((2, chunks, rows, TN), BF),
            pltpu.SemaphoreType.DMA((slots,)),
            pltpu.SemaphoreType.REGULAR,
        ] + [pltpu.SemaphoreType.DMA((2, chunks))] * 4,
        compiler_params=pltpu.CompilerParams(collective_id=ident, has_side_effects=True, vmem_limit_bytes=VMEM),
        name=f"scatter_{ident}",
    )(act, rest, w)


def rotary(tokens):
    half = HEAD // 2
    angle = np.arange(tokens, dtype=np.float32)[:, None] * np.power(np.float32(THETA), -np.arange(half, dtype=np.float32) / half)
    cos, sin = np.cos(angle), np.sin(angle)
    return np.concatenate([cos, cos], 1).astype(np.float32), np.concatenate([-sin, sin], 1).astype(np.float32)


def solution(mesh):
    n = mesh.shape["tp"]

    def step(x, gain_a, wq, wk, wv, wo, gain_m, w_gate, w_up, w_down):
        seen = attention(n, x, gain_a, *rotary(n * x.shape[0]), wq, wk, wv)
        h = added(n, x, seen, wo, 2, paired=True)
        hidden = hidden_units(n, h, gain_m, w_gate, w_up)
        return added(n, h, hidden, w_down, 3)

    tokens, columns, rows_of = P(("dp", "tp"), None), P(None, "tp"), P("tp", None)
    return jax.shard_map(
        step,
        mesh=mesh,
        in_specs=(tokens, P(None), columns, columns, columns, rows_of, P(None), columns, columns, rows_of),
        out_specs=tokens,
        check_vma=False,
    )
```

```python
import functools

import jax
import jax.numpy as jnp
import numpy as np
from jax import lax
from jax.experimental import pallas as pl
from jax.experimental.pallas import tpu as pltpu
from jax.sharding import PartitionSpec as P

HEAD = 128
THETA = 10000
BF, F32 = jnp.bfloat16, jnp.float32
ANY = pl.BlockSpec(memory_space=pl.ANY)
VM = pl.BlockSpec(memory_space=pltpu.VMEM)
CH = 1024
TN = 512
HALF = TN // 2
GROUP = 9
LEAD = 5
HOLD = 12
AHEAD = 2
LAG = 2
VMEM = 63 * 2**20


def _dot(a, b, ca=1, cb=0):
    return lax.dot_general(a, b, (((ca,), (cb,)), ((), ())), preferred_element_type=F32)


def _ring(n):
    me = lax.axis_index("tp")
    return me, lax.rem(me + 1, n), lax.rem(me + n - 1, n), lax.rem(me + 2, n)


def _greet(right, left, other=None):
    barrier = pltpu.get_barrier_semaphore()
    for at in (left, right):
        pl.semaphore_signal(barrier, inc=1, device_id={"tp": at}, device_id_type=pl.DeviceIdType.MESH)
    if other is not None:
        pl.semaphore_signal(barrier, inc=1, device_id={"dp": other}, device_id_type=pl.DeviceIdType.MESH)
    pl.semaphore_wait(barrier, 2 if other is None else 3)


def _send(src, dst, ssem, rsem, to):
    return pltpu.make_async_remote_copy(src_ref=src, dst_ref=dst, send_sem=ssem, recv_sem=rsem, device_id={"tp": to},
                                        device_id_type=pl.DeviceIdType.MESH)


def _loop(a, b, body):
    lax.fori_loop(a, b, lambda i, _: (body(i), None)[1], None)


def _norm_into(x_ref, gain_ref, buf, me, rows):
    chunks = buf.shape[0]
    wide = chunks * CH
    gain = [gain_ref[c * CH : (c + 1) * CH].astype(F32).reshape(1, CH) for c in range(chunks)]

    def body(i):
        at = pl.ds(pl.multiple_of(i * 16, 16), 16)
        total = jnp.zeros((16, CH), F32)
        for c in range(chunks):
            t = x_ref[at, c * CH : (c + 1) * CH].astype(F32)
            total = total + t * t
        scale = lax.rsqrt(jnp.sum(total, -1, keepdims=True) * (1.0 / wide) + 1e-6)
        to = pl.ds(pl.multiple_of(me * rows + i * 16, 16), 16)
        for c in range(chunks):
            t = x_ref[at, c * CH : (c + 1) * CH].astype(F32)
            buf[c, to, :] = (t * scale * gain[c]).astype(BF)

    _loop(0, rows // 16, body)


class _Gather:
    def __init__(self, n, rows, buf, sems):
        self.me, self.right, self.left, self.opp = _ring(n)
        self.rows, self.buf = rows, buf
        self.s_own, self.r_own, self.s_fwd, self.r_fwd = sems

    def _own(self, c, way):
        at = self.buf.at[c, pl.ds(pl.multiple_of(self.me * self.rows, 128), self.rows), :]
        return _send(at, at, self.s_own.at[way, c], self.r_own.at[way, c], self.left if way else self.right)

    def _fwd(self, c, way):
        half = self.rows // 2
        source = self.right if way else self.left
        at = self.buf.at[c, pl.ds(pl.multiple_of(source * self.rows + way * half, half), half), :]
        return _send(at, at, self.s_fwd.at[way, c], self.r_fwd.at[way, c], self.left if way else self.right)

    def start(self, c):
        self._own(c, 0).start()
        self._own(c, 1).start()

    def forward(self, c):
        self._own(c, 0).wait_recv()
        self._fwd(c, 0).start()
        self._own(c, 1).wait_recv()
        self._fwd(c, 1).start()

    def whole(self, c):
        self._fwd(c, 0).wait_recv()
        self._fwd(c, 1).wait_recv()

    def end(self):
        def body(c):
            for way in (0, 1):
                self._own(c, way).wait_send()
                self._fwd(c, way).wait_send()

        _loop(0, self.buf.shape[0], body)


class _Scatter:
    def __init__(self, n, rows, chunks, places, sems):
        self.me, self.right, self.left, self.opp = _ring(n)
        self.rows, self.chunks = rows, chunks
        self.part, self.own, self.s_opp, self.r_opp, self.s_near, self.r_near = places
        self.ss_opp, self.rs_opp, self.ss_near, self.rs_near = sems

    def _far(self, j, way):
        return _send(self.s_opp(way, j), self.r_opp(way, j), self.ss_opp.at[way, j], self.rs_opp.at[way, j], self.left if way else self.right)

    def _near(self, j, way):
        return _send(self.s_near(way, j), self.r_near(way, j), self.ss_near.at[way, j], self.rs_near.at[way, j],
                     self.left if way else self.right)

    def _of(self, j, i, device):
        return self.part(lax.rem(j, LAG + 1), i)[pl.ds(pl.multiple_of(device * self.rows, self.rows), self.rows), :]

    def put(self, j, i, value):
        self.part(lax.rem(j, LAG + 1), i)[...] = value

    def begin(self, j):
        for way in (0, 1):
            self.s_opp(way, j)[...] = self._of(j, way, self.opp).astype(BF)
            self._far(j, way).start()
        for i in (0, 1):
            self.own(j, i)[...] = self._of(j, i, self.me)

        @pl.when(j >= LAG)
        def _():
            self._pass_on(j - LAG)

    def _pass_on(self, j):
        for way, device in ((0, self.right), (1, self.left)):
            self._far(j, way).wait_recv()
            came = self.r_opp(way, j)[...].astype(F32)
            halves = [self._of(j, i, device) for i in (0, 1)]
            halves[way] = halves[way] + came
            self.s_near(way, j)[...] = jnp.concatenate(halves, 1).astype(BF)
            self._near(j, way).start()

    def end(self, rest_ref, out_ref):
        _loop(self.chunks - LAG, self.chunks, self._pass_on)

        def finish(j):
            self._near(j, 0).wait_recv()
            self._near(j, 1).wait_recv()
            at = pl.ds(pl.multiple_of(j * TN, TN), TN)
            total = jnp.concatenate([self.own(j, i)[...] for i in (0, 1)], 1)
            total = total + self.r_near(0, j)[...].astype(F32) + self.r_near(1, j)[...].astype(F32)
            out_ref[:, at] = (rest_ref[:, at].astype(F32) + total).astype(BF)
            for way in (0, 1):
                self._far(j, way).wait_send()
                self._near(j, way).wait_send()

        _loop(0, self.chunks, finish)


def _attention_kernel(n, x_ref, gain_ref, cos_ref, sin_ref, wq_ref, wk_ref, wv_ref, wo_ref, out_ref,
                      buf, acc, w_s, qkv_s, seen_ref, wo_s, part_s, own_s, s_opp, r_opp, s_near, r_near, w_sem, wo_sem, go, go_on,
                      s_own, r_own, s_fwd, r_fwd, ss_opp, rs_opp, ss_near, rs_near):
    group_id = lax.axis_index("dp")
    second = lax.rem(group_id, 2)
    other = group_id + 1 - 2 * second
    rows = x_ref.shape[0]
    chunks, slots = buf.shape[0], w_s.shape[0]
    nq, nk = wq_ref.shape[1], wk_ref.shape[1]
    tokens = n * rows
    total = nq + 2 * nk
    g = _Gather(n, rows, buf, (s_own, r_own, s_fwd, r_fwd))

    def weights(c, slot):
        at = pl.ds(pl.multiple_of(c * CH, CH), CH)
        return [pltpu.make_async_copy(ref.at[at, :], w_s.at[slot, :, lo : lo + size], w_sem.at[slot, i])
                for i, (ref, lo, size) in enumerate(((wq_ref, 0, nq), (wk_ref, nq, nk), (wv_ref, nq + nk, nk)))]

    out_slots = wo_s.shape[0]

    def out_weights(j):
        slot = lax.rem(j, out_slots)
        return pltpu.make_async_copy(wo_ref.at[:, pl.ds(pl.multiple_of(j * TN, TN), TN)], wo_s.at[slot], wo_sem.at[slot])

    for c in range(slots):
        for copy in weights(c, c):
            copy.start()
    for j in range(out_slots):
        out_weights(j).start()
    _norm_into(x_ref, gain_ref, buf, g.me, rows)
    acc[...] = jnp.zeros_like(acc)
    _greet(g.right, g.left, other)

    @pl.when(second == 1)
    def _():
        pl.semaphore_wait(go, 1)

    for c in range(AHEAD + 2):
        g.start(c)
    for c in range(AHEAD):
        g.forward(c)

    def chunk(c):
        @pl.when(c + AHEAD + 2 < chunks)
        def _():
            g.start(c + AHEAD + 2)

        @pl.when(c + AHEAD < chunks)
        def _():
            g.forward(c + AHEAD)

        g.whole(c)

        @pl.when((second == 0) & (c == LEAD))
        def _():
            pl.semaphore_signal(go, inc=1, device_id={"dp": other}, device_id_type=pl.DeviceIdType.MESH)

        slot = lax.rem(c, slots)
        for copy in weights(c, slot):
            copy.wait()

        for lo in range(0, total, 256):
            acc[:, lo : lo + 256] += _dot(buf[c], w_s[slot, :, lo : lo + 256])

        @pl.when(c + slots < chunks)
        def _():
            for copy in weights(c + slots, slot):
                copy.start()

    _loop(0, chunks, chunk)

    def turned(at, of=slice(None)):
        t = acc[of, at].astype(BF).astype(F32)
        return (t * cos_ref[of, :] + pltpu.roll(t, HEAD // 2, 1) * sin_ref[of, :]).astype(BF)

    kv = nk // HEAD
    for i in range(kv):
        qkv_s[i] = turned(slice(nq + i * HEAD, nq + (i + 1) * HEAD))
        qkv_s[kv + i] = acc[:, nq + nk + i * HEAD : nq + nk + (i + 1) * HEAD].astype(BF)
    group = nq // nk
    bq = 128
    hidden = lax.broadcasted_iota(jnp.int32, (bq, bq), 0) < lax.broadcasted_iota(jnp.int32, (bq, bq), 1)

    def heads(pair):
        at = pl.ds(pl.multiple_of(pair * 2 * HEAD, 2 * HEAD), 2 * HEAD)
        i = lax.div(pair * 2, group)
        for b in range(tokens // bq):
            seen = (b + 1) * bq
            outs = []
            for t in range(2):
                q = turned(pl.ds(pl.multiple_of((pair * 2 + t) * HEAD, HEAD), HEAD), slice(b * bq, seen))
                s = _dot(q, qkv_s[i, :seen, :], 1, 1) * (HEAD**-0.5)
                last = jnp.where(hidden, -1e30, s[:, b * bq :])
                s = jnp.concatenate([s[:, : b * bq], last], 1) if b else last
                p = jnp.exp(s - jnp.max(s, -1, keepdims=True))
                out = _dot(p.astype(BF), qkv_s[kv + i, :seen, :]) / jnp.sum(p, -1, keepdims=True)
                outs.append(out.astype(BF))
            seen_ref[b * bq : seen, at] = jnp.concatenate(outs, 1)

    _loop(0, nq // (2 * HEAD), heads)

    sums = wo_ref.shape[1] // TN
    places = (lambda at, i: part_s.at[at, i], lambda j, i: own_s.at[j, i], lambda way, j: s_opp.at[way, j], lambda way, j: r_opp.at[way, j],
              lambda way, j: s_near.at[way, j], lambda way, j: r_near.at[way, j])
    total = _Scatter(n, rows, sums, places, (ss_opp, rs_opp, ss_near, rs_near))

    def out_chunk(j):
        @pl.when((second == 1) & (j == HOLD))
        def _():
            pl.semaphore_signal(go_on, inc=1, device_id={"dp": other}, device_id_type=pl.DeviceIdType.MESH)

        out_weights(j).wait()
        slot = lax.rem(j, out_slots)
        for i in (0, 1):
            total.put(j, i, _dot(seen_ref[...], wo_s[slot, :, i * HALF : (i + 1) * HALF]))

        @pl.when(j + out_slots < sums)
        def _():
            out_weights(j + out_slots).start()

        total.begin(j)

    _loop(0, sums, out_chunk)
    total.end(x_ref, out_ref)
    g.end()

    @pl.when(second == 0)
    def _():
        pl.semaphore_wait(go_on, 1)


def attended(n, x, gain, cos, sin, wq, wk, wv, wo):
    rows, d = x.shape
    nq, nk = wq.shape[1], wk.shape[1]
    chunks, sums = d // CH, d // TN
    slots = 3
    return pl.pallas_call(
        functools.partial(_attention_kernel, n),
        out_shape=jax.ShapeDtypeStruct((rows, d), BF),
        in_specs=[VM, VM, VM, VM, ANY, ANY, ANY, ANY],
        out_specs=VM,
        scratch_shapes=[
            pltpu.VMEM((chunks, n * rows, CH), BF),
            pltpu.VMEM((n * rows, nq + 2 * nk), F32),
            pltpu.VMEM((slots, CH, nq + 2 * nk), BF),
            pltpu.VMEM((2 * nk // HEAD, n * rows, HEAD), BF),
            pltpu.VMEM((n * rows, nq), BF),
            pltpu.VMEM((3, nq, TN), BF),
            pltpu.VMEM((LAG + 1, 2, n * rows, HALF), F32),
            pltpu.VMEM((sums, 2, rows, HALF), F32),
            pltpu.VMEM((2, sums, rows, HALF), BF),
            pltpu.VMEM((2, sums, rows, HALF), BF),
            pltpu.VMEM((2, sums, rows, TN), BF),
            pltpu.VMEM((2, sums, rows, TN), BF),
            pltpu.SemaphoreType.DMA((slots, 3)),
            pltpu.SemaphoreType.DMA((3,)),
            pltpu.SemaphoreType.REGULAR,
            pltpu.SemaphoreType.REGULAR,
        ] + [pltpu.SemaphoreType.DMA((2, chunks))] * 4 + [pltpu.SemaphoreType.DMA((2, sums))] * 4,
        compiler_params=pltpu.CompilerParams(collective_id=0, has_side_effects=True, vmem_limit_bytes=VMEM),
        name="attended",
    )(x, gain, cos, sin, wq, wk, wv, wo)


def _hidden_kernel(n, x_ref, gain_ref, wg_ref, wu_ref, wd_ref, out_ref, buf, acc, w_s, hidden_s, r_opp, r_near, w_sem, d_sem,
                   s_own, r_own, s_fwd, r_fwd, ss_opp, rs_opp, ss_near, rs_near):
    rows = x_ref.shape[0]
    chunks, slots = buf.shape[0], w_s.shape[0]
    full, rest = divmod(wg_ref.shape[1] // 128, GROUP)
    per = full + (rest > 0)
    steps = chunks * per
    g = _Gather(n, rows, buf, (s_own, r_own, s_fwd, r_fwd))

    def weights(s, tiles):
        slot, c, i = lax.rem(s, slots), lax.div(s, per), lax.rem(s, per)
        at = pl.ds(pl.multiple_of(c * CH, CH), CH), pl.ds(pl.multiple_of(i * GROUP * 128, 128), tiles * 128)
        return [pltpu.make_async_copy(ref.at[at], w_s.at[slot, k, :, : tiles * 128], w_sem.at[slot, k])
                for k, ref in enumerate((wg_ref, wu_ref))]

    def fetch(s):
        for yes, tiles in ((lax.rem(s, per) < full, GROUP), (lax.rem(s, per) == full, rest)):
            if tiles:
                @pl.when((s < steps) & yes)
                def _():
                    for copy in weights(s, tiles):
                        copy.start()

    _loop(0, slots, fetch)
    _norm_into(x_ref, gain_ref, buf, g.me, rows)
    _greet(g.right, g.left)
    g.start(0)

    def clear(j):
        acc[j] = jnp.zeros(acc.shape[1:], F32)

    _loop(0, acc.shape[0], clear)
    g.forward(0)
    g.start(1)
    g.start(2)
    g.forward(1)

    def products(c, i, tiles, done):
        s = c * per + i
        slot = lax.rem(s, slots)
        for copy in weights(s, tiles):
            copy.wait()
        for t in range(tiles):
            cols = slice(t * 128, (t + 1) * 128)
            w = jnp.concatenate([w_s[slot, 0, :, cols], w_s[slot, 1, :, cols]], 1)
            j = i * GROUP + t
            done(j, acc[j] + _dot(buf[c], w))
        fetch(s + slots)

    def groups(c, done):
        _loop(0, full, lambda i: products(c, i, GROUP, done))
        if rest:
            products(c, full, rest, done)

    def chunk(c):
        @pl.when(c + 3 < chunks)
        def _():
            g.start(c + 3)

        @pl.when(c + 2 < chunks)
        def _():
            g.forward(c + 2)

        g.whole(c)

        def keep(j, value):
            acc[j] = value

        groups(c, keep)

    _loop(0, chunks - 1, chunk)
    g.whole(chunks - 1)

    def last(j, value):
        gate, up = value[:, :128], value[:, 128:]
        hidden_s[:, pl.ds(pl.multiple_of(j * 128, 128), 128)] = (gate * jax.nn.sigmoid(gate) * up).astype(BF)

    groups(chunks - 1, last)
    g.end()

    deep, sums = wd_ref.shape[0], wd_ref.shape[1] // TN
    blocks = [(b, min(CH, deep - b * CH)) for b in range((deep + CH - 1) // CH)]
    planes = (len(blocks) + 1) // 2
    first = 2 * (steps % slots)

    def plane(j, b):
        flat = lax.rem(first + planes * lax.rem(j, 2) + b // 2, 2 * slots)
        return lax.div(flat, 2), lax.rem(flat, 2), slice((b % 2) * TN, (b % 2 + 1) * TN)

    def down(j):
        cols = pl.ds(pl.multiple_of(j * TN, TN), TN)
        out = []
        for b, size in blocks:
            slot, k, at = plane(j, b)
            out.append(pltpu.make_async_copy(wd_ref.at[b * CH : b * CH + size, cols], w_s.at[slot, k, :size, at], d_sem.at[lax.rem(j, 2), b]))
        return out

    for j in (0, 1):
        for copy in down(j):
            copy.start()

    def place(j, low, high, width):
        at = pl.ds(pl.multiple_of(lax.rem(j, 2) * TN, TN), width)
        return buf.at[lax.div(j, 2), low:high, at]

    places = (lambda at, i: acc.at[2 * at + i],
              lambda j, i: acc.at[2 * (LAG + 1) + lax.div(j, 2), pl.ds(pl.multiple_of((lax.rem(j, 2) * 2 + i) * rows, rows), rows), :],
              lambda way, j: place(j, (2 + way) * rows, (3 + way) * rows, HALF),
              lambda way, j: r_opp.at[way, j],
              lambda way, j: place(j, way * rows, (way + 1) * rows, TN),
              lambda way, j: r_near.at[way, j])
    total = _Scatter(n, rows, sums, places, (ss_opp, rs_opp, ss_near, rs_near))

    def down_chunk(j):
        for copy in down(j):
            copy.wait()
        for i in (0, 1):
            value = None
            for b, size in blocks:
                slot, k, at = plane(j, b)
                t = _dot(hidden_s[:, b * CH : b * CH + size], w_s[slot, k, :size, at.start + i * HALF : at.start + (i + 1) * HALF])
                value = t if value is None else value + t
            total.put(j, i, value)

        @pl.when(j + 2 < sums)
        def _():
            for copy in down(j + 2):
                copy.start()

        total.begin(j)

    _loop(0, sums, down_chunk)
    total.end(x_ref, out_ref)


def hidden_units(n, x, gain, wg, wu, wd):
    rows, d = x.shape
    chunks, sums, tiles, slots = d // CH, d // TN, wg.shape[1] // 128, 3
    blocks = (wd.shape[0] + CH - 1) // CH
    assert (blocks + 1) // 2 * 2 <= 2 * slots and 2 * TN <= GROUP * 128 and 2 * CH >= 2 * TN
    return pl.pallas_call(
        functools.partial(_hidden_kernel, n),
        out_shape=jax.ShapeDtypeStruct((rows, d), BF),
        in_specs=[VM, VM, ANY, ANY, ANY],
        out_specs=VM,
        scratch_shapes=[
            pltpu.VMEM((chunks, n * rows, CH), BF),
            pltpu.VMEM((tiles, n * rows, 256), F32),
            pltpu.VMEM((slots, 2, CH, GROUP * 128), BF),
            pltpu.VMEM((n * rows, wg.shape[1]), BF),
            pltpu.VMEM((2, sums, rows, HALF), BF),
            pltpu.VMEM((2, sums, rows, TN), BF),
            pltpu.SemaphoreType.DMA((slots, 2)),
            pltpu.SemaphoreType.DMA((2, blocks)),
        ] + [pltpu.SemaphoreType.DMA((2, chunks))] * 4 + [pltpu.SemaphoreType.DMA((2, sums))] * 4,
        compiler_params=pltpu.CompilerParams(collective_id=1, has_side_effects=True, vmem_limit_bytes=VMEM),
        name="hidden_units",
    )(x, gain, wg, wu, wd)


def rotary(tokens):
    half = HEAD // 2
    angle = np.arange(tokens, dtype=np.float32)[:, None] * np.power(np.float32(THETA), -np.arange(half, dtype=np.float32) / half)
    cos, sin = np.cos(angle), np.sin(angle)
    return np.concatenate([cos, cos], 1).astype(np.float32), np.concatenate([-sin, sin], 1).astype(np.float32)


def solution(mesh):
    n = mesh.shape["tp"]

    def step(x, gain_a, wq, wk, wv, wo, gain_m, w_gate, w_up, w_down):
        h = attended(n, x, gain_a, *rotary(n * x.shape[0]), wq, wk, wv, wo)
        return hidden_units(n, h, gain_m, w_gate, w_up, w_down)

    tokens, columns, rows_of = P(("dp", "tp"), None), P(None, "tp"), P("tp", None)
    return jax.shard_map(
        step,
        mesh=mesh,
        in_specs=(tokens, P(None), columns, columns, columns, rows_of, P(None), columns, columns, rows_of),
        out_specs=tokens,
        check_vma=False,
    )
```

```python
import functools

import jax
import jax.numpy as jnp
import numpy as np
from jax import lax
from jax.experimental import pallas as pl
from jax.experimental.pallas import tpu as pltpu
from jax.sharding import PartitionSpec as P

HEAD = 128
THETA = 10000
BF, F32 = jnp.bfloat16, jnp.float32
ANY = pl.BlockSpec(memory_space=pl.ANY)
VM = pl.BlockSpec(memory_space=pltpu.VMEM)
CH = 1024
TN = 512
HALF = TN // 2
GROUP = 11
LEAD = 4
HOLD = 14
AHEAD = 2
LAG = 2
VMEM = 63 * 2**20


def _dot(a, b, ca=1, cb=0):
    return lax.dot_general(a, b, (((ca,), (cb,)), ((), ())), preferred_element_type=F32)


def _ring(n):
    me = lax.axis_index("tp")
    return me, lax.rem(me + 1, n), lax.rem(me + n - 1, n), lax.rem(me + 2, n)


def _greet(right, left, other=None):
    barrier = pltpu.get_barrier_semaphore()
    for at in (left, right):
        pl.semaphore_signal(barrier, inc=1, device_id={"tp": at}, device_id_type=pl.DeviceIdType.MESH)
    if other is not None:
        pl.semaphore_signal(barrier, inc=1, device_id={"dp": other}, device_id_type=pl.DeviceIdType.MESH)
    return lambda: pl.semaphore_wait(barrier, 2 if other is None else 3)


def _send(src, dst, ssem, rsem, to):
    return pltpu.make_async_remote_copy(src_ref=src, dst_ref=dst, send_sem=ssem, recv_sem=rsem, device_id={"tp": to},
                                        device_id_type=pl.DeviceIdType.MESH)


def _loop(a, b, body):
    lax.fori_loop(a, b, lambda i, _: (body(i), None)[1], None)


class _Norm:
    def __init__(self, x_ref, gain_ref, scale_s, buf, me):
        self.x_ref, self.gain_ref, self.scale_s, self.buf, self.me = x_ref, gain_ref, scale_s, buf, me
        rows, chunks = x_ref.shape[0], buf.shape[0]

        def body(i):
            at = pl.ds(pl.multiple_of(i * 16, 16), 16)
            total = jnp.zeros((16, CH), F32)
            for c in range(chunks):
                t = x_ref[at, c * CH : (c + 1) * CH].astype(F32)
                total = total + t * t
            scale = lax.rsqrt(jnp.sum(total, -1, keepdims=True) * (1.0 / (chunks * CH)) + 1e-6)
            scale_s[at, :] = jnp.broadcast_to(scale, (16, 128))

        _loop(0, rows // 16, body)

    def chunk(self, c):
        rows = self.x_ref.shape[0]
        gain = self.gain_ref[c * CH : (c + 1) * CH].astype(F32).reshape(1, CH)

        def body(i):
            at = pl.ds(pl.multiple_of(i * 16, 16), 16)
            to = pl.ds(pl.multiple_of(self.me * rows + i * 16, 16), 16)
            t = self.x_ref[at, c * CH : (c + 1) * CH].astype(F32)
            self.buf[c, to, :] = (t * self.scale_s[at, :1] * gain).astype(BF)

        _loop(0, rows // 16, body)


class _Gather:
    def __init__(self, n, rows, buf, sems):
        self.me, self.right, self.left, self.opp = _ring(n)
        self.rows, self.buf = rows, buf
        self.s_own, self.r_own, self.s_fwd, self.r_fwd = sems

    def _own(self, c, way, part):
        half = self.rows // 2
        at = self.buf.at[c, pl.ds(pl.multiple_of(self.me * self.rows + (way ^ part) * half, half), half), :]
        return _send(at, at, self.s_own.at[way, part, c], self.r_own.at[way, part, c], self.left if way else self.right)

    def _fwd(self, c, way):
        half = self.rows // 2
        source = self.right if way else self.left
        at = self.buf.at[c, pl.ds(pl.multiple_of(source * self.rows + way * half, half), half), :]
        return _send(at, at, self.s_fwd.at[way, c], self.r_fwd.at[way, c], self.left if way else self.right)

    def start(self, c):
        for part in (0, 1):
            for way in (0, 1):
                self._own(c, way, part).start()

    def forward(self, c):
        for way in (0, 1):
            self._own(c, way, 0).wait_recv()
            self._fwd(c, way).start()

    def whole(self, c):
        for way in (0, 1):
            self._own(c, way, 1).wait_recv()
            self._fwd(c, way).wait_recv()

    def end(self):
        def body(c):
            for way in (0, 1):
                self._own(c, way, 0).wait_send()
                self._own(c, way, 1).wait_send()
                self._fwd(c, way).wait_send()

        _loop(0, self.buf.shape[0], body)


class _Scatter:
    def __init__(self, n, rows, chunks, places, sems):
        self.me, self.right, self.left, self.opp = _ring(n)
        self.rows, self.chunks = rows, chunks
        self.part, self.own, self.s_opp, self.r_opp, self.s_near, self.r_near = places
        self.ss_opp, self.rs_opp, self.ss_near, self.rs_near = sems

    def _far(self, j, way):
        return _send(self.s_opp(way, j), self.r_opp(way, j), self.ss_opp.at[way, j], self.rs_opp.at[way, j], self.left if way else self.right)

    def _near(self, j, way):
        return _send(self.s_near(way, j), self.r_near(way, j), self.ss_near.at[way, j], self.rs_near.at[way, j],
                     self.left if way else self.right)

    def _of(self, j, i, device):
        return self.part(lax.rem(j, LAG + 1), i)[pl.ds(pl.multiple_of(device * self.rows, self.rows), self.rows), :]

    def put(self, j, i, value):
        self.part(lax.rem(j, LAG + 1), i)[...] = value

    def begin(self, j):
        for way in (0, 1):
            self.s_opp(way, j)[...] = self._of(j, way, self.opp).astype(BF)
            self._far(j, way).start()
        for i in (0, 1):
            self.own(j, i)[...] = self._of(j, i, self.me)

        @pl.when(j >= LAG)
        def _():
            self._pass_on(j - LAG)

    def _pass_on(self, j):
        for way, device in ((0, self.right), (1, self.left)):
            self._far(j, way).wait_recv()
            came = self.r_opp(way, j)[...].astype(F32)
            halves = [self._of(j, i, device) for i in (0, 1)]
            halves[way] = halves[way] + came
            self.s_near(way, j)[...] = jnp.concatenate(halves, 1).astype(BF)
            self._near(j, way).start()

    def end(self, rest_ref, out_ref):
        _loop(self.chunks - LAG, self.chunks, self._pass_on)

        def finish(j):
            self._near(j, 0).wait_recv()
            self._near(j, 1).wait_recv()
            at = pl.ds(pl.multiple_of(j * TN, TN), TN)
            total = jnp.concatenate([self.own(j, i)[...] for i in (0, 1)], 1)
            total = total + self.r_near(0, j)[...].astype(F32) + self.r_near(1, j)[...].astype(F32)
            out_ref[:, at] = (rest_ref[:, at].astype(F32) + total).astype(BF)
            for way in (0, 1):
                self._far(j, way).wait_send()
                self._near(j, way).wait_send()

        _loop(0, self.chunks, finish)


def _attention_kernel(n, x_ref, gain_ref, cos_ref, sin_ref, wq_ref, wk_ref, wv_ref, wo_ref, out_ref,
                      buf, acc, w_s, qkv_s, seen_ref, wo_s, part_s, own_s, s_opp, r_opp, s_near, r_near, scale_s, w_sem, wo_sem, go, go_on,
                      s_own, r_own, s_fwd, r_fwd, ss_opp, rs_opp, ss_near, rs_near):
    group_id = lax.axis_index("dp")
    second = lax.rem(group_id, 2)
    other = group_id + 1 - 2 * second
    rows = x_ref.shape[0]
    chunks, slots = buf.shape[0], w_s.shape[0]
    nq, nk = wq_ref.shape[1], wk_ref.shape[1]
    tokens = n * rows
    total = nq + 2 * nk
    g = _Gather(n, rows, buf, (s_own, r_own, s_fwd, r_fwd))

    greeted = _greet(g.right, g.left, other)

    def weights(c, slot):
        at = pl.ds(pl.multiple_of(c * CH, CH), CH)
        return [pltpu.make_async_copy(ref.at[at, :], w_s.at[slot, :, lo : lo + size], w_sem.at[slot, i])
                for i, (ref, lo, size) in enumerate(((wq_ref, 0, nq), (wk_ref, nq, nk), (wv_ref, nq + nk, nk)))]

    out_slots = wo_s.shape[0]

    def out_weights(j):
        slot = lax.rem(j, out_slots)
        return pltpu.make_async_copy(wo_ref.at[:, pl.ds(pl.multiple_of(j * TN, TN), TN)], wo_s.at[slot], wo_sem.at[slot])

    for c in range(slots):
        for copy in weights(c, c):
            copy.start()
    for j in range(out_slots):
        out_weights(j).start()
    norm = _Norm(x_ref, gain_ref, scale_s, buf, g.me)
    for c in range(AHEAD + 2):
        norm.chunk(c)
    greeted()

    @pl.when(second == 1)
    def _():
        pl.semaphore_wait(go, 1)

    for c in range(AHEAD + 2):
        g.start(c)
    for c in range(AHEAD + 2, chunks):
        norm.chunk(c)
    acc[...] = jnp.zeros_like(acc)
    for c in range(AHEAD):
        g.forward(c)

    def chunk(c):
        @pl.when(c + AHEAD + 2 < chunks)
        def _():
            g.start(c + AHEAD + 2)

        @pl.when(c + AHEAD < chunks)
        def _():
            g.forward(c + AHEAD)

        g.whole(c)

        @pl.when((second == 0) & (c == LEAD))
        def _():
            pl.semaphore_signal(go, inc=1, device_id={"dp": other}, device_id_type=pl.DeviceIdType.MESH)

        slot = lax.rem(c, slots)
        for copy in weights(c, slot):
            copy.wait()

        for lo in range(0, total, 256):
            acc[:, lo : lo + 256] += _dot(buf[c], w_s[slot, :, lo : lo + 256])

        @pl.when(c + slots < chunks)
        def _():
            for copy in weights(c + slots, slot):
                copy.start()

    _loop(0, chunks, chunk)

    def turned(at, of=slice(None)):
        t = acc[of, at].astype(BF).astype(F32)
        return (t * cos_ref[of, :] + pltpu.roll(t, HEAD // 2, 1) * sin_ref[of, :]).astype(BF)

    kv = nk // HEAD
    for i in range(kv):
        qkv_s[i] = turned(slice(nq + i * HEAD, nq + (i + 1) * HEAD))
        qkv_s[kv + i] = acc[:, nq + nk + i * HEAD : nq + nk + (i + 1) * HEAD].astype(BF)
    group = nq // nk
    bq = 128
    hidden = lax.broadcasted_iota(jnp.int32, (bq, bq), 0) < lax.broadcasted_iota(jnp.int32, (bq, bq), 1)

    def heads(pair):
        at = pl.ds(pl.multiple_of(pair * 2 * HEAD, 2 * HEAD), 2 * HEAD)
        i = lax.div(pair * 2, group)
        for b in range(tokens // bq):
            seen = (b + 1) * bq
            outs = []
            for t in range(2):
                q = turned(pl.ds(pl.multiple_of((pair * 2 + t) * HEAD, HEAD), HEAD), slice(b * bq, seen))
                s = _dot(q, qkv_s[i, :seen, :], 1, 1) * (HEAD**-0.5)
                last = jnp.where(hidden, -1e30, s[:, b * bq :])
                s = jnp.concatenate([s[:, : b * bq], last], 1) if b else last
                p = jnp.exp(s - jnp.max(s, -1, keepdims=True))
                out = _dot(p.astype(BF), qkv_s[kv + i, :seen, :]) / jnp.sum(p, -1, keepdims=True)
                outs.append(out.astype(BF))
            seen_ref[b * bq : seen, at] = jnp.concatenate(outs, 1)

    _loop(0, nq // (2 * HEAD), heads)

    sums = wo_ref.shape[1] // TN
    places = (lambda at, i: part_s.at[at, i], lambda j, i: own_s.at[j, i], lambda way, j: s_opp.at[way, j], lambda way, j: r_opp.at[way, j],
              lambda way, j: s_near.at[way, j], lambda way, j: r_near.at[way, j])
    total = _Scatter(n, rows, sums, places, (ss_opp, rs_opp, ss_near, rs_near))

    def out_chunk(j):
        @pl.when((second == 1) & (j == HOLD))
        def _():
            pl.semaphore_signal(go_on, inc=1, device_id={"dp": other}, device_id_type=pl.DeviceIdType.MESH)

        out_weights(j).wait()
        slot = lax.rem(j, out_slots)
        for i in (0, 1):
            total.put(j, i, _dot(seen_ref[...], wo_s[slot, :, i * HALF : (i + 1) * HALF]))

        @pl.when(j + out_slots < sums)
        def _():
            out_weights(j + out_slots).start()

        total.begin(j)

    _loop(0, sums, out_chunk)
    total.end(x_ref, out_ref)
    g.end()

    @pl.when(second == 0)
    def _():
        pl.semaphore_wait(go_on, 1)


def attended(n, x, gain, cos, sin, wq, wk, wv, wo):
    rows, d = x.shape
    nq, nk = wq.shape[1], wk.shape[1]
    chunks, sums = d // CH, d // TN
    slots = 3
    return pl.pallas_call(
        functools.partial(_attention_kernel, n),
        out_shape=jax.ShapeDtypeStruct((rows, d), BF),
        in_specs=[VM, VM, VM, VM, ANY, ANY, ANY, ANY],
        out_specs=VM,
        scratch_shapes=[
            pltpu.VMEM((chunks, n * rows, CH), BF),
            pltpu.VMEM((n * rows, nq + 2 * nk), F32),
            pltpu.VMEM((slots, CH, nq + 2 * nk), BF),
            pltpu.VMEM((2 * nk // HEAD, n * rows, HEAD), BF),
            pltpu.VMEM((n * rows, nq), BF),
            pltpu.VMEM((3, nq, TN), BF),
            pltpu.VMEM((LAG + 1, 2, n * rows, HALF), F32),
            pltpu.VMEM((sums, 2, rows, HALF), F32),
            pltpu.VMEM((2, sums, rows, HALF), BF),
            pltpu.VMEM((2, sums, rows, HALF), BF),
            pltpu.VMEM((2, sums, rows, TN), BF),
            pltpu.VMEM((2, sums, rows, TN), BF),
            pltpu.VMEM((rows, 128), F32),
            pltpu.SemaphoreType.DMA((slots, 3)),
            pltpu.SemaphoreType.DMA((3,)),
            pltpu.SemaphoreType.REGULAR,
            pltpu.SemaphoreType.REGULAR,
        ] + [pltpu.SemaphoreType.DMA((2, 2, chunks))] * 2 + [pltpu.SemaphoreType.DMA((2, chunks))] * 2 + [pltpu.SemaphoreType.DMA((2, sums))] * 4,
        compiler_params=pltpu.CompilerParams(collective_id=0, has_side_effects=True, vmem_limit_bytes=VMEM),
        name="attended",
    )(x, gain, cos, sin, wq, wk, wv, wo)


def _hidden_kernel(n, x_ref, gain_ref, wg_ref, wu_ref, wd_ref, out_ref, buf, acc, w_s, hidden_s, r_opp, r_near, scale_s, w_sem, d_sem,
                   s_own, r_own, s_fwd, r_fwd, ss_opp, rs_opp, ss_near, rs_near):
    rows = x_ref.shape[0]
    chunks, slots = buf.shape[0], w_s.shape[0]
    full, rest = divmod(wg_ref.shape[1] // 128, GROUP)
    per = full + (rest > 0)
    steps = chunks * per
    g = _Gather(n, rows, buf, (s_own, r_own, s_fwd, r_fwd))
    greeted = _greet(g.right, g.left)

    def weights(s, tiles):
        slot, c, i = lax.rem(s, slots), lax.div(s, per), lax.rem(s, per)
        at = pl.ds(pl.multiple_of(c * CH, CH), CH), pl.ds(pl.multiple_of(i * GROUP * 128, 128), tiles * 128)
        return [pltpu.make_async_copy(ref.at[at], w_s.at[slot, k, :, : tiles * 128], w_sem.at[slot, k])
                for k, ref in enumerate((wg_ref, wu_ref))]

    def fetch(s):
        for yes, tiles in ((lax.rem(s, per) < full, GROUP), (lax.rem(s, per) == full, rest)):
            if tiles:
                @pl.when((s < steps) & yes)
                def _():
                    for copy in weights(s, tiles):
                        copy.start()

    _loop(0, slots, fetch)
    norm = _Norm(x_ref, gain_ref, scale_s, buf, g.me)
    norm.chunk(0)
    norm.chunk(1)
    greeted()
    g.start(0)
    for c in range(2, chunks):
        norm.chunk(c)
    g.forward(0)
    g.start(1)
    g.start(2)

    def clear(j):
        acc[j] = jnp.zeros(acc.shape[1:], F32)

    _loop(0, acc.shape[0], clear)
    g.forward(1)

    def products(c, i, tiles, done):
        s = c * per + i
        slot = lax.rem(s, slots)
        for copy in weights(s, tiles):
            copy.wait()
        for t in range(tiles):
            cols = slice(t * 128, (t + 1) * 128)
            w = jnp.concatenate([w_s[slot, 0, :, cols], w_s[slot, 1, :, cols]], 1)
            j = i * GROUP + t
            done(j, acc[j] + _dot(buf[c], w))
        fetch(s + slots)

    def groups(c, done):
        _loop(0, full, lambda i: products(c, i, GROUP, done))
        if rest:
            products(c, full, rest, done)

    def chunk(c):
        @pl.when(c + 3 < chunks)
        def _():
            g.start(c + 3)

        @pl.when(c + 2 < chunks)
        def _():
            g.forward(c + 2)

        g.whole(c)

        def keep(j, value):
            acc[j] = value

        groups(c, keep)

    _loop(0, chunks - 1, chunk)
    g.whole(chunks - 1)

    def last(j, value):
        gate, up = value[:, :128], value[:, 128:]
        hidden_s[:, pl.ds(pl.multiple_of(j * 128, 128), 128)] = (gate * jax.nn.sigmoid(gate) * up).astype(BF)

    groups(chunks - 1, last)
    g.end()

    deep, sums = wd_ref.shape[0], wd_ref.shape[1] // TN
    blocks = [(b, min(CH, deep - b * CH)) for b in range((deep + CH - 1) // CH)]
    planes = (len(blocks) + 1) // 2
    first = 2 * (steps % slots)

    def plane(j, b):
        flat = lax.rem(first + planes * lax.rem(j, 2) + b // 2, 2 * slots)
        return lax.div(flat, 2), lax.rem(flat, 2), slice((b % 2) * TN, (b % 2 + 1) * TN)

    def down(j):
        cols = pl.ds(pl.multiple_of(j * TN, TN), TN)
        out = []
        for b, size in blocks:
            slot, k, at = plane(j, b)
            out.append(pltpu.make_async_copy(wd_ref.at[b * CH : b * CH + size, cols], w_s.at[slot, k, :size, at], d_sem.at[lax.rem(j, 2), b]))
        return out

    for j in (0, 1):
        for copy in down(j):
            copy.start()

    def place(j, low, high, width):
        at = pl.ds(pl.multiple_of(lax.rem(j, 2) * TN, TN), width)
        return buf.at[lax.div(j, 2), low:high, at]

    places = (lambda at, i: acc.at[2 * at + i],
              lambda j, i: acc.at[2 * (LAG + 1) + lax.div(j, 2), pl.ds(pl.multiple_of((lax.rem(j, 2) * 2 + i) * rows, rows), rows), :],
              lambda way, j: place(j, (2 + way) * rows, (3 + way) * rows, HALF),
              lambda way, j: r_opp.at[way, j],
              lambda way, j: place(j, way * rows, (way + 1) * rows, TN),
              lambda way, j: r_near.at[way, j])
    total = _Scatter(n, rows, sums, places, (ss_opp, rs_opp, ss_near, rs_near))

    def down_chunk(j):
        for copy in down(j):
            copy.wait()
        for i in (0, 1):
            value = None
            for b, size in blocks:
                slot, k, at = plane(j, b)
                t = _dot(hidden_s[:, b * CH : b * CH + size], w_s[slot, k, :size, at.start + i * HALF : at.start + (i + 1) * HALF])
                value = t if value is None else value + t
            total.put(j, i, value)

        @pl.when(j + 2 < sums)
        def _():
            for copy in down(j + 2):
                copy.start()

        total.begin(j)

    _loop(0, sums, down_chunk)
    total.end(x_ref, out_ref)


def hidden_units(n, x, gain, wg, wu, wd):
    rows, d = x.shape
    chunks, sums, tiles, slots = d // CH, d // TN, wg.shape[1] // 128, 3
    blocks = (wd.shape[0] + CH - 1) // CH
    assert (blocks + 1) // 2 * 2 <= 2 * slots and 2 * TN <= GROUP * 128 and 2 * CH >= 2 * TN
    return pl.pallas_call(
        functools.partial(_hidden_kernel, n),
        out_shape=jax.ShapeDtypeStruct((rows, d), BF),
        in_specs=[VM, VM, ANY, ANY, ANY],
        out_specs=VM,
        scratch_shapes=[
            pltpu.VMEM((chunks, n * rows, CH), BF),
            pltpu.VMEM((tiles, n * rows, 256), F32),
            pltpu.VMEM((slots, 2, CH, GROUP * 128), BF),
            pltpu.VMEM((n * rows, wg.shape[1]), BF),
            pltpu.VMEM((2, sums, rows, HALF), BF),
            pltpu.VMEM((2, sums, rows, TN), BF),
            pltpu.VMEM((rows, 128), F32),
            pltpu.SemaphoreType.DMA((slots, 2)),
            pltpu.SemaphoreType.DMA((2, blocks)),
        ] + [pltpu.SemaphoreType.DMA((2, 2, chunks))] * 2 + [pltpu.SemaphoreType.DMA((2, chunks))] * 2 + [pltpu.SemaphoreType.DMA((2, sums))] * 4,
        compiler_params=pltpu.CompilerParams(collective_id=1, has_side_effects=True, vmem_limit_bytes=VMEM),
        name="hidden_units",
    )(x, gain, wg, wu, wd)


def rotary(tokens):
    half = HEAD // 2
    angle = np.arange(tokens, dtype=np.float32)[:, None] * np.power(np.float32(THETA), -np.arange(half, dtype=np.float32) / half)
    cos, sin = np.cos(angle), np.sin(angle)
    return np.concatenate([cos, cos], 1).astype(np.float32), np.concatenate([-sin, sin], 1).astype(np.float32)


def solution(mesh):
    n = mesh.shape["tp"]

    def step(x, gain_a, wq, wk, wv, wo, gain_m, w_gate, w_up, w_down):
        h = attended(n, x, gain_a, *rotary(n * x.shape[0]), wq, wk, wv, wo)
        return hidden_units(n, h, gain_m, w_gate, w_up, w_down)

    tokens, columns, rows_of = P(("dp", "tp"), None), P(None, "tp"), P("tp", None)
    return jax.shard_map(
        step,
        mesh=mesh,
        in_specs=(tokens, P(None), columns, columns, columns, rows_of, P(None), columns, columns, rows_of),
        out_specs=tokens,
        check_vma=False,
    )
```

```python
import functools

import jax
import jax.numpy as jnp
import numpy as np
from jax import lax
from jax.experimental import pallas as pl
from jax.experimental.pallas import tpu as pltpu
from jax.sharding import PartitionSpec as P

HEAD = 128
THETA = 10000
BF, F32 = jnp.bfloat16, jnp.float32
ANY = pl.BlockSpec(memory_space=pl.ANY)
VM = pl.BlockSpec(memory_space=pltpu.VMEM)
CH = 1024
TN = 512
HALF = TN // 2
GROUP = 11
LEAD = 4
HOLD = 14
AHEAD = 2
LAG = 2
VMEM = 63 * 2**20


def _dot(a, b, ca=1, cb=0):
    return lax.dot_general(a, b, (((ca,), (cb,)), ((), ())), preferred_element_type=F32)


def _ring(n):
    me = lax.axis_index("tp")
    return me, lax.rem(me + 1, n), lax.rem(me + n - 1, n), lax.rem(me + 2, n)


def _greet(right, left, other=None):
    barrier = pltpu.get_barrier_semaphore()
    for at in (left, right):
        pl.semaphore_signal(barrier, inc=1, device_id={"tp": at}, device_id_type=pl.DeviceIdType.MESH)
    if other is not None:
        pl.semaphore_signal(barrier, inc=1, device_id={"dp": other}, device_id_type=pl.DeviceIdType.MESH)
    return lambda: pl.semaphore_wait(barrier, 2 if other is None else 3)


def _send(src, dst, ssem, rsem, to):
    return pltpu.make_async_remote_copy(src_ref=src, dst_ref=dst, send_sem=ssem, recv_sem=rsem, device_id={"tp": to},
                                        device_id_type=pl.DeviceIdType.MESH)


def _loop(a, b, body):
    lax.fori_loop(a, b, lambda i, _: (body(i), None)[1], None)


class _Norm:
    def __init__(self, x_ref, gain_ref, scale_s, buf, me):
        self.x_ref, self.gain_ref, self.scale_s, self.buf, self.me = x_ref, gain_ref, scale_s, buf, me
        rows, chunks = x_ref.shape[0], buf.shape[0]

        def body(i):
            at = pl.ds(pl.multiple_of(i * 16, 16), 16)
            total = jnp.zeros((16, CH), F32)
            for c in range(chunks):
                t = x_ref[at, c * CH : (c + 1) * CH].astype(F32)
                total = total + t * t
            scale = lax.rsqrt(jnp.sum(total, -1, keepdims=True) * (1.0 / (chunks * CH)) + 1e-6)
            scale_s[at, :] = jnp.broadcast_to(scale, (16, 128))

        _loop(0, rows // 16, body)

    def chunk(self, c):
        rows = self.x_ref.shape[0]
        gain = self.gain_ref[c * CH : (c + 1) * CH].astype(F32).reshape(1, CH)

        def body(i):
            at = pl.ds(pl.multiple_of(i * 16, 16), 16)
            to = pl.ds(pl.multiple_of(self.me * rows + i * 16, 16), 16)
            t = self.x_ref[at, c * CH : (c + 1) * CH].astype(F32)
            self.buf[c, to, :] = (t * self.scale_s[at, :1] * gain).astype(BF)

        _loop(0, rows // 16, body)


class _Gather:
    def __init__(self, n, rows, buf, sems):
        self.me, self.right, self.left, self.opp = _ring(n)
        self.rows, self.buf = rows, buf
        self.s_own, self.r_own, self.s_fwd, self.r_fwd = sems

    def _own(self, c, way, part):
        half = self.rows // 2
        at = self.buf.at[c, pl.ds(pl.multiple_of(self.me * self.rows + (way ^ part) * half, half), half), :]
        return _send(at, at, self.s_own.at[way, part, c], self.r_own.at[way, part, c], self.left if way else self.right)

    def _fwd(self, c, way):
        half = self.rows // 2
        source = self.right if way else self.left
        at = self.buf.at[c, pl.ds(pl.multiple_of(source * self.rows + way * half, half), half), :]
        return _send(at, at, self.s_fwd.at[way, c], self.r_fwd.at[way, c], self.left if way else self.right)

    def start(self, c):
        for part in (0, 1):
            for way in (0, 1):
                self._own(c, way, part).start()

    def forward(self, c):
        for way in (0, 1):
            self._own(c, way, 0).wait_recv()
            self._fwd(c, way).start()

    def whole(self, c):
        for way in (0, 1):
            self._own(c, way, 1).wait_recv()
            self._fwd(c, way).wait_recv()

    def end(self):
        def body(c):
            for way in (0, 1):
                self._own(c, way, 0).wait_send()
                self._own(c, way, 1).wait_send()
                self._fwd(c, way).wait_send()

        _loop(0, self.buf.shape[0], body)


class _Scatter:
    def __init__(self, n, rows, chunks, places, sems):
        self.me, self.right, self.left, self.opp = _ring(n)
        self.rows, self.chunks = rows, chunks
        self.part, self.own, self.s_opp, self.r_opp, self.s_near, self.r_near = places
        self.ss_opp, self.rs_opp, self.ss_near, self.rs_near = sems

    def _far(self, j, way):
        return _send(self.s_opp(way, j), self.r_opp(way, j), self.ss_opp.at[way, j], self.rs_opp.at[way, j], self.left if way else self.right)

    def _near(self, j, way):
        return _send(self.s_near(way, j), self.r_near(way, j), self.ss_near.at[way, j], self.rs_near.at[way, j],
                     self.left if way else self.right)

    def _of(self, j, i, device):
        return self.part(lax.rem(j, LAG + 1), i)[pl.ds(pl.multiple_of(device * self.rows, self.rows), self.rows), :]

    def put(self, j, i, value):
        self.part(lax.rem(j, LAG + 1), i)[...] = value

    def begin(self, j):
        for way in (0, 1):
            self.s_opp(way, j)[...] = self._of(j, way, self.opp).astype(BF)
            self._far(j, way).start()
        for i in (0, 1):
            self.own(j, i)[...] = self._of(j, i, self.me)

        @pl.when(j >= LAG)
        def _():
            self._pass_on(j - LAG)

    def _pass_on(self, j):
        for way, device in ((0, self.right), (1, self.left)):
            self._far(j, way).wait_recv()
            came = self.r_opp(way, j)[...].astype(F32)
            halves = [self._of(j, i, device) for i in (0, 1)]
            halves[way] = halves[way] + came
            self.s_near(way, j)[...] = jnp.concatenate(halves, 1).astype(BF)
            self._near(j, way).start()

    def end(self, rest_ref, out_ref):
        _loop(self.chunks - LAG, self.chunks, self._pass_on)

        def finish(j):
            self._near(j, 0).wait_recv()
            self._near(j, 1).wait_recv()
            at = pl.ds(pl.multiple_of(j * TN, TN), TN)
            total = jnp.concatenate([self.own(j, i)[...] for i in (0, 1)], 1)
            total = total + self.r_near(0, j)[...].astype(F32) + self.r_near(1, j)[...].astype(F32)
            out_ref[:, at] = (rest_ref[:, at].astype(F32) + total).astype(BF)
            for way in (0, 1):
                self._far(j, way).wait_send()
                self._near(j, way).wait_send()

        _loop(0, self.chunks, finish)


def _attention_kernel(n, x_ref, gain_ref, cos_ref, sin_ref, wq_ref, wk_ref, wv_ref, wo_ref, out_ref,
                      buf, acc, w_s, qkv_s, seen_ref, wo_s, part_s, own_s, s_opp, r_opp, s_near, r_near, scale_s, w_sem, wo_sem, go, go_on,
                      s_own, r_own, s_fwd, r_fwd, ss_opp, rs_opp, ss_near, rs_near):
    group_id = lax.axis_index("dp")
    second = lax.rem(group_id, 2)
    other = group_id + 1 - 2 * second
    rows = x_ref.shape[0]
    chunks, slots = buf.shape[0], w_s.shape[0]
    nq, nk = wq_ref.shape[1], wk_ref.shape[1]
    tokens = n * rows
    total = nq + 2 * nk
    g = _Gather(n, rows, buf, (s_own, r_own, s_fwd, r_fwd))

    greeted = _greet(g.right, g.left, other)

    def weights(c, slot):
        at = pl.ds(pl.multiple_of(c * CH, CH), CH)
        return [pltpu.make_async_copy(ref.at[at, :], w_s.at[slot, :, lo : lo + size], w_sem.at[slot, i])
                for i, (ref, lo, size) in enumerate(((wq_ref, 0, nq), (wk_ref, nq, nk), (wv_ref, nq + nk, nk)))]

    out_slots = wo_s.shape[0]

    def out_weights(j):
        slot = lax.rem(j, out_slots)
        return pltpu.make_async_copy(wo_ref.at[:, pl.ds(pl.multiple_of(j * TN, TN), TN)], wo_s.at[slot], wo_sem.at[slot])

    for c in range(slots):
        for copy in weights(c, c):
            copy.start()
    for j in range(out_slots):
        out_weights(j).start()
    norm = _Norm(x_ref, gain_ref, scale_s, buf, g.me)
    for c in range(AHEAD + 2):
        norm.chunk(c)
    greeted()

    @pl.when(second == 1)
    def _():
        pl.semaphore_wait(go, 1)

    for c in range(AHEAD + 2):
        g.start(c)
    for c in range(AHEAD + 2, chunks):
        norm.chunk(c)
    acc[...] = jnp.zeros_like(acc)
    for c in range(AHEAD):
        g.forward(c)

    def chunk(c):
        @pl.when(c + AHEAD + 2 < chunks)
        def _():
            g.start(c + AHEAD + 2)

        @pl.when(c + AHEAD < chunks)
        def _():
            g.forward(c + AHEAD)

        g.whole(c)

        @pl.when((second == 0) & (c == LEAD))
        def _():
            pl.semaphore_signal(go, inc=1, device_id={"dp": other}, device_id_type=pl.DeviceIdType.MESH)

        slot = lax.rem(c, slots)
        for copy in weights(c, slot):
            copy.wait()

        for lo in range(0, total, 256):
            acc[:, lo : lo + 256] += _dot(buf[c], w_s[slot, :, lo : lo + 256])

        @pl.when(c + slots < chunks)
        def _():
            for copy in weights(c + slots, slot):
                copy.start()

    _loop(0, chunks, chunk)

    def turned(at, of=slice(None)):
        t = acc[of, at].astype(BF).astype(F32)
        return (t * cos_ref[of, :] + pltpu.roll(t, HEAD // 2, 1) * sin_ref[of, :]).astype(BF)

    kv = nk // HEAD
    for i in range(kv):
        qkv_s[i] = turned(slice(nq + i * HEAD, nq + (i + 1) * HEAD))
        qkv_s[kv + i] = acc[:, nq + nk + i * HEAD : nq + nk + (i + 1) * HEAD].astype(BF)
    group = nq // nk
    bq = 128
    hidden = lax.broadcasted_iota(jnp.int32, (bq, bq), 0) < lax.broadcasted_iota(jnp.int32, (bq, bq), 1)

    def heads(pair):
        at = pl.ds(pl.multiple_of(pair * 2 * HEAD, 2 * HEAD), 2 * HEAD)
        i = lax.div(pair * 2, group)
        for b in range(tokens // bq):
            seen = (b + 1) * bq
            outs = []
            for t in range(2):
                q = turned(pl.ds(pl.multiple_of((pair * 2 + t) * HEAD, HEAD), HEAD), slice(b * bq, seen))
                s = _dot(q, qkv_s[i, :seen, :], 1, 1) * (HEAD**-0.5)
                last = jnp.where(hidden, -1e30, s[:, b * bq :])
                s = jnp.concatenate([s[:, : b * bq], last], 1) if b else last
                p = jnp.exp(s - jnp.max(s, -1, keepdims=True))
                out = _dot(p.astype(BF), qkv_s[kv + i, :seen, :]) / jnp.sum(p, -1, keepdims=True)
                outs.append(out.astype(BF))
            seen_ref[b * bq : seen, at] = jnp.concatenate(outs, 1)

    _loop(0, nq // (2 * HEAD), heads)

    sums = wo_ref.shape[1] // TN
    places = (lambda at, i: part_s.at[at, i], lambda j, i: own_s.at[j, i], lambda way, j: s_opp.at[way, j], lambda way, j: r_opp.at[way, j],
              lambda way, j: s_near.at[way, j], lambda way, j: r_near.at[way, j])
    total = _Scatter(n, rows, sums, places, (ss_opp, rs_opp, ss_near, rs_near))

    def out_chunk(j):
        @pl.when((second == 1) & (j == HOLD))
        def _():
            pl.semaphore_signal(go_on, inc=1, device_id={"dp": other}, device_id_type=pl.DeviceIdType.MESH)

        out_weights(j).wait()
        slot = lax.rem(j, out_slots)
        for i in (0, 1):
            total.put(j, i, _dot(seen_ref[...], wo_s[slot, :, i * HALF : (i + 1) * HALF]))

        @pl.when(j + out_slots < sums)
        def _():
            out_weights(j + out_slots).start()

        total.begin(j)

    _loop(0, sums, out_chunk)
    total.end(x_ref, out_ref)
    g.end()

    @pl.when(second == 0)
    def _():
        pl.semaphore_wait(go_on, 1)


def attended(n, x, gain, cos, sin, wq, wk, wv, wo):
    rows, d = x.shape
    nq, nk = wq.shape[1], wk.shape[1]
    chunks, sums = d // CH, d // TN
    slots = 3
    return pl.pallas_call(
        functools.partial(_attention_kernel, n),
        out_shape=jax.ShapeDtypeStruct((rows, d), BF),
        in_specs=[VM, VM, VM, VM, ANY, ANY, ANY, ANY],
        out_specs=VM,
        scratch_shapes=[
            pltpu.VMEM((chunks, n * rows, CH), BF),
            pltpu.VMEM((n * rows, nq + 2 * nk), F32),
            pltpu.VMEM((slots, CH, nq + 2 * nk), BF),
            pltpu.VMEM((2 * nk // HEAD, n * rows, HEAD), BF),
            pltpu.VMEM((n * rows, nq), BF),
            pltpu.VMEM((3, nq, TN), BF),
            pltpu.VMEM((LAG + 1, 2, n * rows, HALF), F32),
            pltpu.VMEM((sums, 2, rows, HALF), F32),
            pltpu.VMEM((2, sums, rows, HALF), BF),
            pltpu.VMEM((2, sums, rows, HALF), BF),
            pltpu.VMEM((2, sums, rows, TN), BF),
            pltpu.VMEM((2, sums, rows, TN), BF),
            pltpu.VMEM((rows, 128), F32),
            pltpu.SemaphoreType.DMA((slots, 3)),
            pltpu.SemaphoreType.DMA((3,)),
            pltpu.SemaphoreType.REGULAR,
            pltpu.SemaphoreType.REGULAR,
        ] + [pltpu.SemaphoreType.DMA((2, 2, chunks))] * 2 + [pltpu.SemaphoreType.DMA((2, chunks))] * 2 + [pltpu.SemaphoreType.DMA((2, sums))] * 4,
        compiler_params=pltpu.CompilerParams(collective_id=0, has_side_effects=True, vmem_limit_bytes=VMEM),
        name="attended",
    )(x, gain, cos, sin, wq, wk, wv, wo)


def _hidden_kernel(n, x_ref, gain_ref, wg_ref, wu_ref, wd_ref, out_ref, buf, acc, w_s, hidden_s, r_opp, r_near, scale_s, w_sem, d_sem,
                   s_own, r_own, s_fwd, r_fwd, ss_opp, rs_opp, ss_near, rs_near):
    rows = x_ref.shape[0]
    chunks, slots = buf.shape[0], w_s.shape[0]
    full, rest = divmod(wg_ref.shape[1] // 128, GROUP)
    per = full + (rest > 0)
    steps = chunks * per
    g = _Gather(n, rows, buf, (s_own, r_own, s_fwd, r_fwd))
    greeted = _greet(g.right, g.left)

    def weights(s, tiles):
        slot, c, i = lax.rem(s, slots), lax.div(s, per), lax.rem(s, per)
        at = pl.ds(pl.multiple_of(c * CH, CH), CH), pl.ds(pl.multiple_of(i * GROUP * 128, 128), tiles * 128)
        return [pltpu.make_async_copy(ref.at[at], w_s.at[slot, k, :, : tiles * 128], w_sem.at[slot, k])
                for k, ref in enumerate((wg_ref, wu_ref))]

    def fetch(s):
        for yes, tiles in ((lax.rem(s, per) < full, GROUP), (lax.rem(s, per) == full, rest)):
            if tiles:
                @pl.when((s < steps) & yes)
                def _():
                    for copy in weights(s, tiles):
                        copy.start()

    _loop(0, slots, fetch)
    norm = _Norm(x_ref, gain_ref, scale_s, buf, g.me)
    norm.chunk(0)
    norm.chunk(1)
    greeted()
    g.start(0)
    for c in range(2, chunks):
        norm.chunk(c)
    g.forward(0)
    g.start(1)
    g.start(2)

    def clear(j):
        acc[j] = jnp.zeros(acc.shape[1:], F32)

    _loop(0, acc.shape[0], clear)
    g.forward(1)

    def products(c, i, tiles, done):
        s = c * per + i
        slot = lax.rem(s, slots)
        for copy in weights(s, tiles):
            copy.wait()
        for t in range(tiles):
            cols = slice(t * 128, (t + 1) * 128)
            w = jnp.concatenate([w_s[slot, 0, :, cols], w_s[slot, 1, :, cols]], 1)
            j = i * GROUP + t
            done(j, acc[j] + _dot(buf[c], w))
        fetch(s + slots)

    def groups(c, done, ahead=None):
        _loop(0, full, lambda i: products(c, i, GROUP, done))
        if ahead:
            ahead()
        if rest:
            products(c, full, rest, done)

    def chunk(c):
        @pl.when(c + 3 < chunks)
        def _():
            g.start(c + 3)

        @pl.when(c + 2 < chunks)
        def _():
            g.forward(c + 2)

        g.whole(c)

        def keep(j, value):
            acc[j] = value

        groups(c, keep)

    _loop(0, chunks - 1, chunk)
    g.whole(chunks - 1)

    def last(j, value):
        gate, up = value[:, :128], value[:, 128:]
        hidden_s[:, pl.ds(pl.multiple_of(j * 128, 128), 128)] = (gate * jax.nn.sigmoid(gate) * up).astype(BF)

    deep, sums = wd_ref.shape[0], wd_ref.shape[1] // TN
    blocks = [(b, min(CH, deep - b * CH)) for b in range((deep + CH - 1) // CH)]
    planes = (len(blocks) + 1) // 2
    first = 2 * (steps % slots)

    def plane(j, b):
        flat = lax.rem(first + planes * lax.rem(j, 2) + b // 2, 2 * slots)
        return lax.div(flat, 2), lax.rem(flat, 2), slice((b % 2) * TN, (b % 2 + 1) * TN)

    def down(j):
        cols = pl.ds(pl.multiple_of(j * TN, TN), TN)
        out = []
        for b, size in blocks:
            slot, k, at = plane(j, b)
            out.append(pltpu.make_async_copy(wd_ref.at[b * CH : b * CH + size, cols], w_s.at[slot, k, :size, at], d_sem.at[lax.rem(j, 2), b]))
        return out

    def fetch_down(j):
        for copy in down(j):
            copy.start()

    groups(chunks - 1, last, lambda: fetch_down(0))
    g.end()

    fetch_down(1)

    def place(j, low, high, width):
        at = pl.ds(pl.multiple_of(lax.rem(j, 2) * TN, TN), width)
        return buf.at[lax.div(j, 2), low:high, at]

    places = (lambda at, i: acc.at[2 * at + i],
              lambda j, i: acc.at[2 * (LAG + 1) + lax.div(j, 2), pl.ds(pl.multiple_of((lax.rem(j, 2) * 2 + i) * rows, rows), rows), :],
              lambda way, j: place(j, (2 + way) * rows, (3 + way) * rows, HALF),
              lambda way, j: r_opp.at[way, j],
              lambda way, j: place(j, way * rows, (way + 1) * rows, TN),
              lambda way, j: r_near.at[way, j])
    total = _Scatter(n, rows, sums, places, (ss_opp, rs_opp, ss_near, rs_near))

    def down_chunk(j):
        for copy in down(j):
            copy.wait()
        for i in (0, 1):
            value = None
            for b, size in blocks:
                slot, k, at = plane(j, b)
                t = _dot(hidden_s[:, b * CH : b * CH + size], w_s[slot, k, :size, at.start + i * HALF : at.start + (i + 1) * HALF])
                value = t if value is None else value + t
            total.put(j, i, value)

        @pl.when(j + 2 < sums)
        def _():
            for copy in down(j + 2):
                copy.start()

        total.begin(j)

    _loop(0, sums, down_chunk)
    total.end(x_ref, out_ref)


def hidden_units(n, x, gain, wg, wu, wd):
    rows, d = x.shape
    chunks, sums, tiles, slots = d // CH, d // TN, wg.shape[1] // 128, 3
    blocks = (wd.shape[0] + CH - 1) // CH
    assert slots == 3 and (blocks + 1) // 2 <= slots and 2 * TN <= GROUP * 128 and 2 * CH >= 2 * TN
    return pl.pallas_call(
        functools.partial(_hidden_kernel, n),
        out_shape=jax.ShapeDtypeStruct((rows, d), BF),
        in_specs=[VM, VM, ANY, ANY, ANY],
        out_specs=VM,
        scratch_shapes=[
            pltpu.VMEM((chunks, n * rows, CH), BF),
            pltpu.VMEM((tiles, n * rows, 256), F32),
            pltpu.VMEM((slots, 2, CH, GROUP * 128), BF),
            pltpu.VMEM((n * rows, wg.shape[1]), BF),
            pltpu.VMEM((2, sums, rows, HALF), BF),
            pltpu.VMEM((2, sums, rows, TN), BF),
            pltpu.VMEM((rows, 128), F32),
            pltpu.SemaphoreType.DMA((slots, 2)),
            pltpu.SemaphoreType.DMA((2, blocks)),
        ] + [pltpu.SemaphoreType.DMA((2, 2, chunks))] * 2 + [pltpu.SemaphoreType.DMA((2, chunks))] * 2 + [pltpu.SemaphoreType.DMA((2, sums))] * 4,
        compiler_params=pltpu.CompilerParams(collective_id=1, has_side_effects=True, vmem_limit_bytes=VMEM),
        name="hidden_units",
    )(x, gain, wg, wu, wd)


def rotary(tokens):
    half = HEAD // 2
    angle = np.arange(tokens, dtype=np.float32)[:, None] * np.power(np.float32(THETA), -np.arange(half, dtype=np.float32) / half)
    cos, sin = np.cos(angle), np.sin(angle)
    return np.concatenate([cos, cos], 1).astype(np.float32), np.concatenate([-sin, sin], 1).astype(np.float32)


def solution(mesh):
    n = mesh.shape["tp"]

    def step(x, gain_a, wq, wk, wv, wo, gain_m, w_gate, w_up, w_down):
        h = attended(n, x, gain_a, *rotary(n * x.shape[0]), wq, wk, wv, wo)
        return hidden_units(n, h, gain_m, w_gate, w_up, w_down)

    tokens, columns, rows_of = P(("dp", "tp"), None), P(None, "tp"), P("tp", None)
    return jax.shard_map(
        step,
        mesh=mesh,
        in_specs=(tokens, P(None), columns, columns, columns, rows_of, P(None), columns, columns, rows_of),
        out_specs=tokens,
        check_vma=False,
    )
```
